128 devices in a mesh: ctx: 16 (over y, x), tp: 8 (over z, core).
Axes of the slice: x: 4, y: 4, z: 4, core: 2. Of those that a mesh axis runs over, the one named last changes fastest.
Arguments:
- hidden: bfloat16 [8, 8192], P(None, 'ctx'), may hold values from -4.8 to 4.8, as said below
- norm_gains: bfloat16 [4, 8192], P(None, 'ctx'), may hold values from 0.5 to 1.5
- w_query: bfloat16 [4, 8192, 8192], P(None, 'ctx', 'tp'), may hold values from -0.0625 to 0.0625
- w_key: bfloat16 [4, 8192, 1024], P(None, 'ctx', 'tp'), may hold values from -0.125 to 0.125
- w_value: bfloat16 [4, 8192, 1024], P(None, 'ctx', 'tp'), may hold values from -0.125 to 0.125
- w_out: bfloat16 [4, 8192, 8192], P(None, 'tp', 'ctx'), may hold values from -0.0625 to 0.0625
- key_cache: bfloat16 [4, 8, 8, 2048, 128], P(None, None, 'tp', 'ctx'), may hold values from -9 to 9
- value_cache: bfloat16 [4, 8, 8, 2048, 128], P(None, None, 'tp', 'ctx'), may hold values from -6 to 6
- lengths: int32 [8], replicated, may hold values from 1 to 2048, 8200 in all
Outputs:
- updated: float32 [8, 8192], P(None, 'ctx')
The draws below stay inside these ranges and needn't reach their ends.
Inputs may be any that keep to these rules, and one draw needn't show every extreme that they name: Each sequence has lengths[b] valid cache positions 0 .. lengths[b] - 1, between 1 and 2048; the longest sequence has exactly 2048; the new token sits at position lengths[b]. `hidden`: activations of order 0.2; in each block of 512 consecutive features one sequence, chosen at random, has entries four times larger.
All inputs are finite; a program needn't handle non-finite values.
Results may differ from the reference program's by a relative error of at most 0.02.
Values sent between devices are 32-bit elements.
A program may use at most 64 MiB of HBM per device.

```python
import math
import jax
import jax.numpy as jnp
import numpy as np
from jax import lax

D = 8192
HQ = 64
KVH = 8
HD = 128
LAYERS = 4
BATCH = 8
CAP = 2048
D_DEV = 512


def draw_hidden(key, part):
    base_key, owner_key = jax.random.split(jax.random.fold_in(key, 7))
    block_count = D // D_DEV
    owners = jax.random.randint(owner_key, (block_count,), 0, BATCH)
    column_owner = owners[jnp.arange(D) // D_DEV]
    factor = jnp.where(column_owner[None, :] == jnp.arange(BATCH)[:, None], 4.0, 1.0)
    base_draw = jnp.clip(jax.random.normal(base_key, (BATCH, D), jnp.float32), -6.0, 6.0)
    return (0.2 * factor * base_draw).astype(jnp.bfloat16)


def block_scale(rng, extent, pieces, smallest, high):
    gain = 1.0
    for axis_at, parts in pieces:
        draws = jax.random.uniform(jax.random.fold_in(jax.random.fold_in(rng, 6), axis_at), (parts,), jnp.float32, smallest / len(pieces), high / len(pieces))
        gain = gain * jnp.repeat(jnp.exp(draws), extent[axis_at] // parts).reshape((-1,) + (1,) * (len(extent) - 1 - axis_at))
    return gain


def profile(count, total, reach, slope):
    portions = [(1 << 20) // math.isqrt(grade ** slope) + 1 for grade in range(2, count + 1)]
    surplus, given = total - reach - (count - 1), [1] * (count - 1)
    while surplus > 0:
        movable = [i for i in range(count - 1) if given[i] < reach]
        mass, remaining = sum([portions[i] for i in movable]), surplus
        for i in movable:
            extra = min(reach - given[i], max(1, remaining * portions[i] // mass), surplus)
            given[i] = given[i] + extra
            surplus = surplus - extra
    return np.array([reach] + given)


def ragged(rng, amount, total, most, lean):
    if amount == 2:
        one = jax.random.randint(rng, (), max(1, total - most), min(most, total - 1) + 1)
        return jnp.stack([one, total - one])
    sizes = jnp.asarray(profile(amount, total, most, lean), jnp.int32)
    couples = (amount - 1) // 2
    source_of, taker = sizes[1:1 + 2 * couples:2], sizes[2:2 + 2 * couples:2]
    slack = jnp.minimum(source_of - 1, most - taker)
    shifted = jax.random.randint(jax.random.fold_in(rng, 1), (couples,), 0, 1 << 20) % (slack + 1)
    sizes = sizes.at[1:1 + 2 * couples:2].set(source_of - shifted).at[2:2 + 2 * couples:2].set(taker + shifted)
    return sizes[jax.random.permutation(jax.random.fold_in(rng, 2), amount)]


def scatter_about(stream_key, dims, scale, limit, pieces=(), kind=jnp.bfloat16):
    array = scale * jax.random.normal(stream_key, dims, jnp.float32)
    if pieces:
        array = array * block_scale(stream_key, dims, pieces, -0.22, 0.18)
    return jnp.clip(array, -limit, limit).astype(kind)


def setup_inputs(seed: int = 0) -> dict:
    key_list = jax.random.split(jax.random.key(seed), 10)
    hidden = draw_hidden(jax.random.fold_in(key_list[9], 71), 0)
    norm_gains = jnp.clip(1.0 + 0.1 * jax.random.normal(key_list[1], (LAYERS, D), jnp.float32), 0.5, 1.5).astype(jnp.bfloat16)
    w_query = scatter_about(key_list[2], (LAYERS, D, HQ * HD), D ** -0.5, 0.0625, ((1, 16), (2, 8)))
    w_key = scatter_about(key_list[3], (LAYERS, D, KVH * HD), (D // 4) ** -0.5, 0.125, ((1, 16), (2, 8)))
    w_value = scatter_about(key_list[4], (LAYERS, D, KVH * HD), (D // 4) ** -0.5, 0.125, ((1, 16), (2, 8)))
    w_out = scatter_about(key_list[5], (LAYERS, HQ * HD, D), (HQ * HD) ** -0.5, 0.0625, ((1, 8), (2, 16)))
    key_cache = scatter_about(key_list[6], (LAYERS, BATCH, KVH, CAP, HD), 1.5, 9.0, ((2, 8), (3, 16)))
    value_cache = scatter_about(key_list[7], (LAYERS, BATCH, KVH, CAP, HD), 1.0, 6.0, ((2, 8), (3, 16)))
    lengths = ragged(key_list[8], BATCH, BATCH * CAP // 2 + BATCH, CAP, 2).astype(jnp.int32)
    return dict(hidden=hidden, norm_gains=norm_gains, w_query=w_query, w_key=w_key, w_value=w_value, w_out=w_out, key_cache=key_cache, value_cache=value_cache, lengths=lengths)


mask_fill = -1e+30
norm_eps = 1e-05
rope_base = 500000.0

def rotate(vectors, positions):
    width = vectors.shape[-1]
    half_width = width // 2
    exponents = jnp.arange(half_width, dtype=jnp.float32) * (2.0 / width)
    frequency = jnp.exp(-exponents * math.log(rope_base))
    angles = positions.astype(jnp.float32)[:, None] * frequency[None, :]
    cosine = jnp.cos(angles)[:, None, :]
    sine_part = jnp.sin(angles)[:, None, :]
    first_half = vectors[..., :half_width]
    second_half = vectors[..., half_width:]
    return jnp.concatenate([first_half * cosine - second_half * sine_part, second_half * cosine + first_half * sine_part], axis=-1)

def reference(hidden, norm_gains, w_query, w_key, w_value, w_out, key_cache, value_cache, lengths):
    stream = hidden.astype(jnp.float32)
    group_size = HQ // KVH
    logit_multiplier = 1.0 / math.sqrt(HD)
    positions = jnp.arange(CAP, dtype=jnp.int32)
    usable = (positions[None, :] < lengths[:, None])[:, None, None, :]
    for layer_idx in range(LAYERS):
        reciprocal_value = lax.rsqrt(lax.optimization_barrier(jnp.sum(stream * stream, axis=1)) / D + norm_eps)
        scaled = (stream * norm_gains[layer_idx].astype(jnp.float32)).astype(jnp.bfloat16)
        raw_query = jnp.dot(scaled, w_query[layer_idx], preferred_element_type=jnp.float32)
        raw_key = jnp.dot(scaled, w_key[layer_idx], preferred_element_type=jnp.float32)
        raw_value = jnp.dot(scaled, w_value[layer_idx], preferred_element_type=jnp.float32)
        query = rotate((raw_query * reciprocal_value[:, None]).reshape(BATCH, HQ, HD), lengths).astype(jnp.bfloat16)
        fresh_lookup_vector = rotate((raw_key * reciprocal_value[:, None]).reshape(BATCH, KVH, HD), lengths).astype(jnp.bfloat16)
        new_value = (raw_value * reciprocal_value[:, None]).reshape(BATCH, KVH, HD).astype(jnp.bfloat16)
        shared_head_sets = query.reshape(BATCH, KVH, group_size, HD).astype(jnp.float32)
        scores = jnp.einsum('bkgd,bksd->bkgs', shared_head_sets, key_cache[layer_idx].astype(jnp.float32), precision=lax.Precision.HIGHEST) * logit_multiplier
        self_match_logit = jnp.einsum('uryj,urj->ury', shared_head_sets, fresh_lookup_vector.astype(jnp.float32), precision=lax.Precision.HIGHEST) * logit_multiplier
        masked = jnp.where(usable, scores, mask_fill)
        largest = jnp.maximum(lax.optimization_barrier(jnp.max(masked, axis=-1)), self_match_logit)
        attention_probabilities = jnp.where(usable, jnp.exp(masked - largest[..., None]), 0.0)
        fresh = jnp.exp(self_match_logit - largest)
        nearest_whole = lax.optimization_barrier(attention_probabilities.astype(jnp.bfloat16)).astype(jnp.float32)
        fresh_rounded = lax.optimization_barrier(fresh.astype(jnp.bfloat16)).astype(jnp.float32)
        numerator = jnp.einsum('bkgs,bksd->bkgd', nearest_whole, value_cache[layer_idx].astype(jnp.float32), precision=lax.Precision.HIGHEST)
        numerator = numerator + fresh_rounded[..., None] * new_value.astype(jnp.float32)[:, :, None, :]
        denominator = lax.optimization_barrier(jnp.sum(attention_probabilities, axis=-1)) + fresh
        context = (numerator / denominator[..., None]).reshape(BATCH, HQ * HD).astype(jnp.bfloat16)
        stream = stream + jnp.dot(context, w_out[layer_idx], preferred_element_type=jnp.float32)
    return stream
```

```python
import functools
import math

import jax
import jax.numpy as jnp
import numpy as np
from jax import lax
from jax.experimental import pallas as pl
from jax.experimental.pallas import tpu as pltpu
from jax.sharding import PartitionSpec as P

MESH = pl.DeviceIdType.MESH
LAYERS = 4
B = 8
HD = 128
HALF = 64
D = 8192
SEG = 128
FILL = -1e30
EPS = 1e-5
ROPE_BASE = 500000.0
F32 = jnp.float32
BF16 = jnp.bfloat16
QA = 5 * HD
QB = 5 * HD
PART = 6 * HD


def tile(value, i):
    return value[:, i * HD : (i + 1) * HD]


def kernel(
    hidden, gains, w_query, w_key, w_value, w_out, key_cache, value_cache, lengths, freq,
    out,
    hbuf, gbuf, wqkv, wo, kbuf, vbuf, fbuf, snd, rcv, tpb,
    lsem, psem, fsem, ssem, rsem, tssem, trsem,
):
    c = lax.axis_index("ctx")
    t = lax.axis_index("tp")
    y, x = c // 4, lax.rem(c, 4)

    def weight_loads(l):
        return (
            pltpu.make_async_copy(w_query.at[l], wqkv.at[l, :, pl.ds(0, 8 * HD)], lsem.at[l, 0]),
            pltpu.make_async_copy(w_key.at[l], wqkv.at[l, :, pl.ds(8 * HD, HD)], lsem.at[l, 1]),
            pltpu.make_async_copy(w_value.at[l], wqkv.at[l, :, pl.ds(9 * HD, HD)], lsem.at[l, 2]),
            pltpu.make_async_copy(key_cache.at[l, :, 0], kbuf.at[l], lsem.at[l, 3]),
            pltpu.make_async_copy(value_cache.at[l, :, 0], vbuf.at[l], lsem.at[l, 4]),
            pltpu.make_async_copy(w_out.at[l], wo.at[l], lsem.at[l, 5]),
        )

    small = (
        pltpu.make_async_copy(hidden, hbuf, psem.at[0]),
        pltpu.make_async_copy(gains, gbuf, psem.at[1]),
        pltpu.make_async_copy(freq, fbuf, psem.at[2]),
    )
    for copy in small:
        copy.start()
    loads = [weight_loads(l) for l in range(LAYERS)]
    for group in loads:
        for copy in group:
            copy.start()

    along_x = [(y * 4 + lax.rem(x + d, 4), t) for d in (1, 2, 3)]
    along_y = [(lax.rem(y + d, 4) * 4 + x, t) for d in (1, 2, 3)]
    along_t = [(c, lax.rem(t + d, 8)) for d in range(1, 8)]
    barrier = pltpu.get_barrier_semaphore()
    for peer in along_x + along_y + along_t:
        pl.semaphore_signal(barrier, inc=1, device_id=peer, device_id_type=MESH)

    lane = lax.broadcasted_iota(jnp.int32, (B, HD), 1)
    row = lax.broadcasted_iota(jnp.int32, (B, HD), 0)
    length = jnp.zeros((B, HD), jnp.int32)
    for b in range(B):
        length = jnp.where(row == b, lengths[b], length)
    usable = c * SEG + lane < length
    small[2].wait()
    angle = length.astype(F32) * fbuf[...]
    cosine = jnp.cos(angle)
    sine = jnp.where(lane < HALF, -jnp.sin(angle), jnp.sin(angle))
    small[0].wait()
    small[1].wait()
    stream = hbuf[...].astype(F32)
    pl.semaphore_wait(barrier, 13)

    def exchange(l, phase, width, peers):
        copies = []
        for i in (1, 0, 2):
            copy = pltpu.make_async_remote_copy(
                src_ref=snd.at[l, phase, :, pl.ds(0, width)],
                dst_ref=rcv.at[l, phase, i, :, pl.ds(0, width)],
                send_sem=ssem.at[l, phase, i],
                recv_sem=rsem.at[l, phase, i],
                device_id=peers[i],
                device_id_type=MESH,
            )
            copy.start()
            copies.append(copy)
        return copies

    def arrive(copies):
        for copy in copies:
            copy.wait_recv()

    def total(l, phase, width):
        own = snd[l, phase, :, :width]
        got = [rcv[l, phase, i, :, :width] for i in range(3)]
        return (own + got[0]) + (got[1] + got[2])

    def merge(l, phase, fresh=None):
        outs = [snd[l, phase, :, : 4 * HD]] + [rcv[l, phase, i, :, : 4 * HD] for i in range(3)]
        stats = [snd[l, phase, :, 4 * HD : 5 * HD]] + [
            rcv[l, phase, i, :, 4 * HD : 5 * HD] for i in range(3)
        ]
        sums = [pltpu.roll(s, HALF, 1) for s in stats]
        top = jnp.maximum(jnp.maximum(stats[0], stats[1]), jnp.maximum(stats[2], stats[3]))
        if fresh is not None:
            top = jnp.maximum(top, fresh[0])
        scale = [jnp.exp(s - top) for s in stats]
        whole = (scale[0] * sums[0] + scale[1] * sums[1]) + (scale[2] * sums[2] + scale[3] * sums[3])
        if fresh is not None:
            new = jnp.exp(fresh[0] - top)
            whole = whole + new
            scale = [s / whole for s in scale]
            new = new.astype(BF16).astype(F32) / whole
        result = []
        for j in range(4):
            parts = [jnp.broadcast_to(s[:, j : j + 1], (B, HD)) * tile(o, j) for s, o in zip(scale, outs)]
            joined = (parts[0] + parts[1]) + (parts[2] + parts[3])
            if fresh is not None:
                joined = joined + jnp.broadcast_to(new[:, j : j + 1], (B, HD)) * fresh[1]
            result.append(joined)
        return result, top, whole

    sent = []
    for l in range(LAYERS):
        load = loads[l]
        gain = gbuf[l : l + 1, :].astype(F32)
        scaled = (stream * gain).astype(BF16)
        squares = stream * stream
        squares = (tile(squares, 0) + tile(squares, 1)) + (tile(squares, 2) + tile(squares, 3))
        for i in range(3):
            load[i].wait()
        snd[l, 0, :, :QA] = jnp.dot(scaled, wqkv[l, :, :QA], preferred_element_type=F32)
        snd[l, 0, :, QA : QA + HD] = squares
        a1 = exchange(l, 0, QA + HD, along_x)
        snd[l, 1, :, :QB] = jnp.dot(scaled, wqkv[l, :, QA:], preferred_element_type=F32)
        b1 = exchange(l, 1, QB, along_y)
        arrive(a1)
        snd[l, 2, :, : QA + HD] = total(l, 0, QA + HD)
        a2 = exchange(l, 2, QA + HD, along_y)
        arrive(b1)
        snd[l, 3, :, :QB] = total(l, 1, QB)
        b2 = exchange(l, 3, QB, along_x)
        load[3].wait()
        load[4].wait()
        arrive(a2)
        first = total(l, 2, QA + HD)
        inverse = lax.rsqrt(jnp.sum(tile(first, 5), axis=1, keepdims=True) / D + EPS)
        cos_l, sin_l = cosine * inverse, sine * inverse

        def rotate(u):
            return u * cos_l + pltpu.roll(u, HALF, 1) * sin_l

        arrive(b2)
        second = total(l, 3, QB)
        raw = [tile(first, i) for i in range(5)] + [tile(second, i) for i in range(3)]
        query = jnp.concatenate([rotate(u) for u in raw], axis=0).astype(BF16)
        new_key = rotate(tile(second, 3)).astype(BF16).astype(F32)
        new_value = (tile(second, 4) * inverse).astype(BF16).astype(F32)

        keys = kbuf[l].reshape(B * SEG, HD)
        score = lax.dot_general(query, keys, (((1,), (1,)), ((), ())), preferred_element_type=F32)
        probs, tops, sums = [], [], []
        for h in range(8):
            block = score[h * B : (h + 1) * B]
            s = tile(block, 0)
            for b in range(1, B):
                s = jnp.where(row == b, tile(block, b), s)
            s = jnp.where(usable, s * (1.0 / math.sqrt(HD)), FILL)
            top = jnp.max(s, axis=1, keepdims=True)
            p = jnp.where(usable, jnp.exp(s - top), 0.0)
            tops.append(top)
            sums.append(jnp.sum(p, axis=1, keepdims=True))
            probs.append(jnp.concatenate([jnp.where(row == b, p, 0.0) for b in range(B)], axis=1))
        probs = jnp.concatenate(probs, axis=0).astype(BF16)
        mixed = jnp.dot(probs, vbuf[l].reshape(B * SEG, HD), preferred_element_type=F32)

        def store_half(phase, start):
            stats = jnp.zeros((B, HD), F32)
            for j in range(4):
                h = start + j
                snd[l, phase, :, j * HD : (j + 1) * HD] = mixed[h * B : (h + 1) * B]
                stats = jnp.where(lane == j, tops[h], stats)
                stats = jnp.where(lane == HALF + j, sums[h], stats)
            snd[l, phase, :, 4 * HD : 5 * HD] = stats

        store_half(4, 0)
        a3 = exchange(l, 4, 5 * HD, along_x)
        store_half(5, 4)
        b3 = exchange(l, 5, 5 * HD, along_y)
        own = [jnp.zeros((B, HD), F32), jnp.zeros((B, HD), F32)]
        for h in range(8):
            dot = jnp.sum(query[h * B : (h + 1) * B].astype(F32) * new_key, axis=1, keepdims=True)
            own[h // 4] = jnp.where(lane == h % 4, dot * (1.0 / math.sqrt(HD)), own[h // 4])

        def pass_on(phase_in, phase_out):
            joined, top, whole = merge(l, phase_in)
            for j in range(4):
                snd[l, phase_out, :, j * HD : (j + 1) * HD] = joined[j]
            snd[l, phase_out, :, 4 * HD : 5 * HD] = jnp.where(lane < HALF, top, pltpu.roll(whole, HALF, 1))

        arrive(a3)
        pass_on(4, 6)
        a4 = exchange(l, 6, 5 * HD, along_y)
        arrive(b3)
        pass_on(5, 7)
        b4 = exchange(l, 7, 5 * HD, along_x)
        load[5].wait()
        arrive(a4)
        context = jnp.concatenate(merge(l, 6, (own[0], new_value))[0], axis=1).astype(BF16)
        head_part = jnp.dot(context, wo[l, : 4 * HD, :], preferred_element_type=F32)
        arrive(b4)
        context = jnp.concatenate(merge(l, 7, (own[1], new_value))[0], axis=1).astype(BF16)
        head_part = head_part + jnp.dot(context, wo[l, 4 * HD :, :], preferred_element_type=F32)

        tpb[l, t] = head_part
        copies = []
        for d in (4, 5, 3, 2, 6, 1, 7):
            copy = pltpu.make_async_remote_copy(
                src_ref=tpb.at[l, t],
                dst_ref=tpb.at[l, t],
                send_sem=tssem.at[l, d - 1],
                recv_sem=trsem.at[l, d - 1],
                device_id=along_t[d - 1],
                device_id_type=MESH,
            )
            copy.start()
            copies.append(copy)
        sent += a1 + b1 + a2 + b2 + a3 + b3 + a4 + b4 + copies
        arrive(copies)
        gathered = [tpb[l, i] for i in range(8)]
        while len(gathered) > 1:
            gathered = [gathered[i] + gathered[i + 1] for i in range(0, len(gathered), 2)]
        stream = stream + gathered[0]
    out[...] = stream
    for copy in sent:
        copy.wait_send()


def on_device(hidden, norm_gains, w_query, w_key, w_value, w_out, key_cache, value_cache, lengths):
    exponents = np.arange(HALF, dtype=np.float32) * np.float32(2.0 / HD)
    freq = np.exp(-exponents.astype(np.float64) * math.log(ROPE_BASE)).astype(np.float32)
    freq = jnp.asarray(np.tile(np.concatenate([freq, freq])[None, :], (B, 1)))
    hbm = pl.BlockSpec(memory_space=pl.ANY)
    return pl.pallas_call(
        kernel,
        out_shape=jax.ShapeDtypeStruct((B, 512), F32),
        in_specs=[hbm] * 8 + [pl.BlockSpec(memory_space=pltpu.SMEM), hbm],
        out_specs=pl.BlockSpec(memory_space=pltpu.VMEM),
        scratch_shapes=[
            pltpu.VMEM((B, 512), BF16),
            pltpu.VMEM((LAYERS, 512), BF16),
            pltpu.VMEM((LAYERS, 512, 10 * HD), BF16),
            pltpu.VMEM((LAYERS, 8 * HD, 512), BF16),
            pltpu.VMEM((LAYERS, B, SEG, HD), BF16),
            pltpu.VMEM((LAYERS, B, SEG, HD), BF16),
            pltpu.VMEM((B, HD), F32),
            pltpu.VMEM((LAYERS, 8, B, PART), F32),
            pltpu.VMEM((LAYERS, 8, 3, B, PART), F32),
            pltpu.VMEM((LAYERS, 8, B, 512), F32),
            pltpu.SemaphoreType.DMA((LAYERS, 6)),
            pltpu.SemaphoreType.DMA((3,)),
            pltpu.SemaphoreType.DMA((1,)),
            pltpu.SemaphoreType.DMA((LAYERS, 8, 3)),
            pltpu.SemaphoreType.DMA((LAYERS, 8, 3)),
            pltpu.SemaphoreType.DMA((LAYERS, 7)),
            pltpu.SemaphoreType.DMA((LAYERS, 7)),
        ],
        compiler_params=pltpu.CompilerParams(
            collective_id=0, has_side_effects=True, vmem_limit_bytes=60 * 1024 * 1024
        ),
    )(hidden, norm_gains, w_query, w_key, w_value, w_out, key_cache, value_cache, lengths, freq)


def solution(mesh):
    return jax.shard_map(
        on_device,
        mesh=mesh,
        in_specs=(
            P(None, "ctx"),
            P(None, "ctx"),
            P(None, "ctx", "tp"),
            P(None, "ctx", "tp"),
            P(None, "ctx", "tp"),
            P(None, "tp", "ctx"),
            P(None, None, "tp", "ctx", None),
            P(None, None, "tp", "ctx", None),
            P(),
        ),
        out_specs=P(None, "ctx"),
        check_vma=False,
    )
```

```python
import functools
import math

import jax
import jax.numpy as jnp
import numpy as np
from jax import lax
from jax.experimental import pallas as pl
from jax.experimental.pallas import tpu as pltpu
from jax.sharding import PartitionSpec as P

MESH = pl.DeviceIdType.MESH
LAYERS = 4
B = 8
HD = 128
HALF = 64
D = 8192
SEG = 128
FILL = -1e30
EPS = 1e-5
ROPE_BASE = 500000.0
F32 = jnp.float32
BF16 = jnp.bfloat16
QA = 5 * HD
QB = 5 * HD
PART = 6 * HD
PLANE_ORDER = (10, 6, 9, 11, 14, 2, 8, 5, 7, 13, 15, 1, 3, 4, 12)
UNIT = 32
PLAN = (2, 1, 2, 1, 3, 3, 2, 2, 2, 2, 2, 2, 0, 0)


def tile(value, i):
    return value[:, i * HD : (i + 1) * HD]


def add_up(terms):
    while len(terms) > 1:
        pairs = [terms[i] + terms[i + 1] for i in range(0, len(terms) - 1, 2)]
        terms = pairs + terms[len(terms) - len(terms) % 2 :]
    return terms[0]


def kernel(
    hidden, gains, w_query, w_key, w_value, w_out, key_cache, value_cache, lengths, freq,
    out,
    hbuf, gbuf, wqkv, wo, kbuf, vbuf, fbuf, snd, rcv, tpb, keys_t, stage, moved, values, qsnd, qrcv, orcv,
    lsem, psem, ssem, rsem, tssem, trsem, bssem, brsem, qssem, qrsem, ossem, orsem,
):
    c = lax.axis_index("ctx")
    t = lax.axis_index("tp")
    y, x = c // 4, lax.rem(c, 4)
    mine, part = lax.rem(c, 8), c // 8

    def weight_loads(l):
        return (
            pltpu.make_async_copy(w_query.at[l], wqkv.at[l, :, pl.ds(0, 8 * HD)], lsem.at[l, 0]),
            pltpu.make_async_copy(w_key.at[l], wqkv.at[l, :, pl.ds(8 * HD, HD)], lsem.at[l, 1]),
            pltpu.make_async_copy(w_value.at[l], wqkv.at[l, :, pl.ds(9 * HD, HD)], lsem.at[l, 2]),
            pltpu.make_async_copy(key_cache.at[l, :, 0], kbuf.at[l], lsem.at[l, 3]),
            pltpu.make_async_copy(value_cache.at[l, :, 0], vbuf.at[l], lsem.at[l, 4]),
            pltpu.make_async_copy(w_out.at[l], wo.at[l], lsem.at[l, 5]),
        )

    small = (
        pltpu.make_async_copy(hidden, hbuf, psem.at[0]),
        pltpu.make_async_copy(gains, gbuf, psem.at[1]),
        pltpu.make_async_copy(freq, fbuf, psem.at[2]),
    )
    for copy in small:
        copy.start()
    loads = [weight_loads(l) for l in range(LAYERS)]
    for group in loads:
        for copy in group:
            copy.start()

    along_x = [(y * 4 + lax.rem(x + d, 4), t) for d in (1, 2, 3)]
    along_y = [(lax.rem(y + d, 4) * 4 + x, t) for d in (1, 2, 3)]
    along_t = [(c, lax.rem(t + d, 8)) for d in range(1, 8)]
    plane = [(lax.rem(y + d // 4, 4) * 4 + lax.rem(x + d % 4, 4), t) for d in range(1, 16)]
    barrier = pltpu.get_barrier_semaphore()
    for peer in plane + along_t:
        pl.semaphore_signal(barrier, inc=1, device_id=peer, device_id_type=MESH)

    lane = lax.broadcasted_iota(jnp.int32, (B, HD), 1)
    row = lax.broadcasted_iota(jnp.int32, (B, HD), 0)
    length = jnp.zeros((B, HD), jnp.int32)
    for b in range(B):
        length = jnp.where(row == b, lengths[b], length)
    usable = c * SEG + lane < length
    my_length = lengths[mine]
    small[2].wait()

    def angles(positions):
        angle = positions.astype(F32) * fbuf[...]
        sine = jnp.sin(angle)
        return jnp.cos(angle), jnp.where(lane < HALF, -sine, sine)

    cosine, sine = angles(length)
    my_cosine, my_sine = angles(jnp.full((B, HD), my_length, jnp.int32))
    small[0].wait()
    small[1].wait()
    stream = hbuf[...].astype(F32)
    pl.semaphore_wait(barrier, 22)

    def exchange(l, phase, width, peers):
        copies = []
        for i in (1, 0, 2):
            copy = pltpu.make_async_remote_copy(
                src_ref=snd.at[l, phase, :, pl.ds(0, width)],
                dst_ref=rcv.at[l, phase, i, :, pl.ds(0, width)],
                send_sem=ssem.at[l, phase, i],
                recv_sem=rsem.at[l, phase, i],
                device_id=peers[i],
                device_id_type=MESH,
            )
            copy.start()
            copies.append(copy)
        return copies

    def arrive(copies):
        for copy in copies:
            copy.wait_recv()

    def total(l, phase, width):
        own = snd[l, phase, :, :width]
        got = [rcv[l, phase, i, :, :width] for i in range(3)]
        return (own + got[0]) + (got[1] + got[2])

    def merge(l, phase, fresh=None):
        outs = [snd[l, phase, :, : 4 * HD]] + [rcv[l, phase, i, :, : 4 * HD] for i in range(3)]
        stats = [snd[l, phase, :, 4 * HD : 5 * HD]] + [
            rcv[l, phase, i, :, 4 * HD : 5 * HD] for i in range(3)
        ]
        sums = [pltpu.roll(s, HALF, 1) for s in stats]
        top = jnp.maximum(jnp.maximum(stats[0], stats[1]), jnp.maximum(stats[2], stats[3]))
        if fresh is not None:
            top = jnp.maximum(top, fresh[0])
        scale = [jnp.exp(s - top) for s in stats]
        whole = (scale[0] * sums[0] + scale[1] * sums[1]) + (scale[2] * sums[2] + scale[3] * sums[3])
        if fresh is not None:
            new = jnp.exp(fresh[0] - top)
            whole = whole + new
            scale = [s / whole for s in scale]
            new = new.astype(BF16).astype(F32) / whole
        result = []
        for j in range(4):
            parts = [jnp.broadcast_to(s[:, j : j + 1], (B, HD)) * tile(o, j) for s, o in zip(scale, outs)]
            joined = (parts[0] + parts[1]) + (parts[2] + parts[3])
            if fresh is not None:
                joined = joined + jnp.broadcast_to(new[:, j : j + 1], (B, HD)) * fresh[1]
            result.append(joined)
        return result, top, whole


    def widen(l):
        loads[l][3].wait()
        loads[l][4].wait()
        for b in range(B):
            stage[l - 1, b, 0] = kbuf[l, b].astype(F32)
            stage[l - 1, b, 1] = vbuf[l, b].astype(F32)
        moved[l - 1, mine, 0] = stage[l - 1, mine, 0]
        moved[l - 1, mine, 1] = stage[l - 1, mine, 1]

    def move(l, unit):
        which, rows = unit // (SEG // UNIT), pl.ds(unit % (SEG // UNIT) * UNIT, UNIT)
        for d in (1, 4, 2, 6, 3, 5, 7):
            to = lax.rem(mine + d, 8)
            pltpu.make_async_remote_copy(
                src_ref=stage.at[l - 1, to, which, rows],
                dst_ref=moved.at[l - 1, mine, which, rows],
                send_sem=bssem.at[l - 1, d - 1],
                recv_sem=brsem.at[l - 1, d - 1],
                device_id=(part * 8 + to, t),
                device_id_type=MESH,
            ).start()

    def moves(l):
        result = []
        for d in range(1, 8):
            origin = lax.rem(mine + 8 - d, 8)
            result.append(
                pltpu.make_async_remote_copy(
                    src_ref=stage.at[l - 1, lax.rem(mine + d, 8)],
                    dst_ref=moved.at[l - 1, origin],
                    send_sem=bssem.at[l - 1, d - 1],
                    recv_sem=brsem.at[l - 1, d - 1],
                    device_id=(part * 8 + lax.rem(mine + d, 8), t),
                    device_id_type=MESH,
                )
            )
        return result

    def narrow(l):
        arrive(moves(l))
        for s in range(8):
            keys_t[l, :, s * SEG : (s + 1) * SEG] = moved[l - 1, s, 0].T.astype(BF16)
            values[l - 1, s * SEG : (s + 1) * SEG] = moved[l - 1, s, 1].astype(BF16)

    queue = [(l, u) for l in range(1, LAYERS) for u in range(2 * SEG // UNIT)]

    def background():
        for _ in range(min(PLAN[len(steps)], len(queue))):
            l, u = queue.pop(0)
            if u == 0:
                widen(l)
            move(l, u)
        steps.append(1)

    steps = []
    sent = []

    within = part * 1024 + lax.broadcasted_iota(jnp.int32, (B, 1024), 1) < my_length

    def first_layer(l, load, scaled, squares):
        nonlocal sent
        snd[l, 0, :, :QA] = jnp.dot(scaled, wqkv[l, :, :QA], preferred_element_type=F32)
        snd[l, 0, :, QA : QA + HD] = squares
        a1 = exchange(l, 0, QA + HD, along_x)
        snd[l, 1, :, :QB] = jnp.dot(scaled, wqkv[l, :, QA:], preferred_element_type=F32)
        b1 = exchange(l, 1, QB, along_y)
        load[3].wait()
        load[4].wait()
        for b in range(B):
            keys_t[0, :, b * SEG : (b + 1) * SEG] = kbuf[0, b].astype(F32).T.astype(BF16)
        background()
        arrive(a1)
        snd[l, 2, :, : QA + HD] = total(l, 0, QA + HD)
        a2 = exchange(l, 2, QA + HD, along_y)
        arrive(b1)
        snd[l, 3, :, :QB] = total(l, 1, QB)
        b2 = exchange(l, 3, QB, along_x)
        background()
        arrive(a2)
        first = total(l, 2, QA + HD)
        inverse = lax.rsqrt(jnp.sum(tile(first, 5), axis=1, keepdims=True) / D + EPS)
        cos_l, sin_l = cosine * inverse, sine * inverse

        def rotate(u):
            return u * cos_l + pltpu.roll(u, HALF, 1) * sin_l

        arrive(b2)
        second = total(l, 3, QB)
        raw = [tile(first, i) for i in range(5)] + [tile(second, i) for i in range(3)]
        query = jnp.concatenate([rotate(u) for u in raw], axis=0).astype(BF16)
        new_key = rotate(tile(second, 3)).astype(BF16).astype(F32)
        new_value = (tile(second, 4) * inverse).astype(BF16).astype(F32)

        score = jnp.dot(query, keys_t[l], preferred_element_type=F32)
        probs, tops, sums = [], [], []
        for h in range(8):
            block = score[h * B : (h + 1) * B]
            s = tile(block, 0)
            for b in range(1, B):
                s = jnp.where(row == b, tile(block, b), s)
            s = jnp.where(usable, s * (1.0 / math.sqrt(HD)), FILL)
            top = jnp.max(s, axis=1, keepdims=True)
            p = jnp.where(usable, jnp.exp(s - top), 0.0)
            tops.append(top)
            sums.append(jnp.sum(p, axis=1, keepdims=True))
            probs.append(jnp.concatenate([jnp.where(row == b, p, 0.0) for b in range(B)], axis=1))
        probs = jnp.concatenate(probs, axis=0).astype(BF16)
        mixed = jnp.dot(probs, vbuf[l].reshape(B * SEG, HD), preferred_element_type=F32)

        def store_half(phase, start):
            stats = jnp.zeros((B, HD), F32)
            for j in range(4):
                h = start + j
                snd[l, phase, :, j * HD : (j + 1) * HD] = mixed[h * B : (h + 1) * B]
                stats = jnp.where(lane == j, tops[h], stats)
                stats = jnp.where(lane == HALF + j, sums[h], stats)
            snd[l, phase, :, 4 * HD : 5 * HD] = stats

        store_half(4, 0)
        a3 = exchange(l, 4, 5 * HD, along_x)
        store_half(5, 4)
        b3 = exchange(l, 5, 5 * HD, along_y)
        background()
        own = [jnp.zeros((B, HD), F32), jnp.zeros((B, HD), F32)]
        for h in range(8):
            dot = jnp.sum(query[h * B : (h + 1) * B].astype(F32) * new_key, axis=1, keepdims=True)
            own[h // 4] = jnp.where(lane == h % 4, dot * (1.0 / math.sqrt(HD)), own[h // 4])

        def pass_on(phase_in, phase_out):
            joined, top, whole = merge(l, phase_in)
            for j in range(4):
                snd[l, phase_out, :, j * HD : (j + 1) * HD] = joined[j]
            snd[l, phase_out, :, 4 * HD : 5 * HD] = jnp.where(lane < HALF, top, pltpu.roll(whole, HALF, 1))

        arrive(a3)
        pass_on(4, 6)
        a4 = exchange(l, 6, 5 * HD, along_y)
        arrive(b3)
        pass_on(5, 7)
        b4 = exchange(l, 7, 5 * HD, along_x)
        background()
        load[5].wait()
        arrive(a4)
        context = jnp.concatenate(merge(l, 6, (own[0], new_value))[0], axis=1).astype(BF16)
        head_part = jnp.dot(context, wo[l, : 4 * HD, :], preferred_element_type=F32)
        arrive(b4)
        context = jnp.concatenate(merge(l, 7, (own[1], new_value))[0], axis=1).astype(BF16)
        head_part = head_part + jnp.dot(context, wo[l, 4 * HD :, :], preferred_element_type=F32)
        sent += a1 + b1 + a2 + b2 + a3 + b3 + a4 + b4
        return head_part

    def later_layer(l, load, scaled, squares):
        nonlocal sent

        raw = jnp.dot(scaled, wqkv[l], preferred_element_type=F32)
        for i in range(10):
            qsnd[l - 1, pl.ds(i, B, stride=16), :] = tile(raw, i)
        qsnd[l - 1, pl.ds(10, B, stride=16), :] = squares
        copies = []
        for d in PLANE_ORDER:
            to = plane[d - 1]
            rows = pl.ds(pl.multiple_of(lax.rem(to[0], 8) * 16, 16), 11)
            copy = pltpu.make_async_remote_copy(
                src_ref=qsnd.at[l - 1, rows],
                dst_ref=qrcv.at[l - 1, d - 1, pl.ds(0, 11)],
                send_sem=qssem.at[l - 1, d - 1],
                recv_sem=qrsem.at[l - 1, d - 1],
                device_id=to,
                device_id_type=MESH,
            )
            copy.start()
            copies.append(copy)
        sent += copies
        background()
        narrow(l)
        at = pl.multiple_of(mine * 16, 16)
        heads = [qsnd[l - 1, pl.ds(at, 8), :]]
        others = [qsnd[l - 1, pl.ds(at + 8, 3), :]]
        arrive(copies)
        for d in range(15):
            heads.append(qrcv[l - 1, d, 0:8, :])
            others.append(qrcv[l - 1, d, 8:11, :])
        heads, others = add_up(heads), add_up(others)
        inverse = lax.rsqrt(jnp.sum(others[2:3], axis=1, keepdims=True) / D + EPS)

        def rotate(u, rows):
            u = u * inverse
            return u * my_cosine[:rows] + pltpu.roll(u, HALF, 1) * my_sine[:rows]

        query = rotate(heads, 8).astype(BF16)
        new_key = rotate(jnp.broadcast_to(others[0:1], (B, HD)), 8).astype(BF16).astype(F32)
        new_value = (others[1:2] * inverse).astype(BF16).astype(F32)
        scale = 1.0 / math.sqrt(HD)
        score = jnp.dot(query, keys_t[l], preferred_element_type=F32)
        own = jnp.sum(query.astype(F32) * new_key, axis=1, keepdims=True) * scale
        own = jnp.where(part == 0, own, FILL)
        score = jnp.where(within, score * scale, FILL)
        top = jnp.maximum(jnp.max(score, axis=1, keepdims=True), own)
        p = jnp.where(within, jnp.exp(score - top), 0.0)
        fresh = jnp.where(part == 0, jnp.exp(own - top), 0.0)
        weight = jnp.sum(p, axis=1, keepdims=True) + fresh
        mixed = jnp.dot(p.astype(BF16), values[l - 1], preferred_element_type=F32)
        mixed = mixed + fresh.astype(BF16).astype(F32) * new_value
        stats = jnp.where(lane == row, top, 0.0) + jnp.where(lane == row + HALF, weight, 0.0)
        base = pl.multiple_of(c * 16, 16)
        orcv[l - 1, pl.ds(base, 8), :] = mixed
        orcv[l - 1, pl.ds(base + 8, 1), :] = jnp.sum(stats, axis=0, keepdims=True)
        copies = []
        for d in PLANE_ORDER:
            copy = pltpu.make_async_remote_copy(
                src_ref=orcv.at[l - 1, pl.ds(base, 9)],
                dst_ref=orcv.at[l - 1, pl.ds(base, 9)],
                send_sem=ossem.at[l - 1, d - 1],
                recv_sem=orsem.at[l - 1, d - 1],
                device_id=plane[d - 1],
                device_id_type=MESH,
            )
            copy.start()
            copies.append(copy)
        sent += copies
        background()
        load[5].wait()
        arrive(copies)
        low = orcv[l - 1, pl.ds(8, B, stride=16), :]
        high = orcv[l - 1, pl.ds(128 + 8, B, stride=16), :]
        top = jnp.maximum(low, high)
        scales = [jnp.exp(low - top), jnp.exp(high - top)]
        whole = scales[0] * pltpu.roll(low, HALF, 1) + scales[1] * pltpu.roll(high, HALF, 1)
        scales = [s / whole for s in scales]
        context = []
        for h in range(8):
            context.append(
                jnp.broadcast_to(scales[0][:, h : h + 1], (B, HD)) * orcv[l - 1, pl.ds(h, B, stride=16), :]
                + jnp.broadcast_to(scales[1][:, h : h + 1], (B, HD)) * orcv[l - 1, pl.ds(128 + h, B, stride=16), :]
            )
        context = jnp.concatenate(context, axis=1).astype(BF16)
        return jnp.dot(context, wo[l], preferred_element_type=F32)

    for l in range(LAYERS):
        load = loads[l]
        gain = gbuf[l : l + 1, :].astype(F32)
        scaled = (stream * gain).astype(BF16)
        squares = stream * stream
        squares = (tile(squares, 0) + tile(squares, 1)) + (tile(squares, 2) + tile(squares, 3))
        for i in range(3):
            load[i].wait()
        head_part = (first_layer if l == 0 else later_layer)(l, load, scaled, squares)

        tpb[l, t] = head_part
        copies = []
        for d in (4, 5, 3, 2, 6, 1, 7):
            copy = pltpu.make_async_remote_copy(
                src_ref=tpb.at[l, t],
                dst_ref=tpb.at[l, t],
                send_sem=tssem.at[l, d - 1],
                recv_sem=trsem.at[l, d - 1],
                device_id=along_t[d - 1],
                device_id_type=MESH,
            )
            copy.start()
            copies.append(copy)
        sent += copies
        background()
        arrive(copies)
        stream = stream + add_up([tpb[l, i] for i in range(8)])
    out[...] = stream
    for l in range(1, LAYERS):
        sent += moves(l)
    for copy in sent:
        copy.wait_send()


def on_device(hidden, norm_gains, w_query, w_key, w_value, w_out, key_cache, value_cache, lengths):
    exponents = np.arange(HALF, dtype=np.float32) * np.float32(2.0 / HD)
    freq = np.exp(-exponents.astype(np.float64) * math.log(ROPE_BASE)).astype(np.float32)
    freq = jnp.asarray(np.tile(np.concatenate([freq, freq])[None, :], (B, 1)))
    hbm = pl.BlockSpec(memory_space=pl.ANY)
    return pl.pallas_call(
        kernel,
        out_shape=jax.ShapeDtypeStruct((B, 512), F32),
        in_specs=[hbm] * 8 + [pl.BlockSpec(memory_space=pltpu.SMEM), hbm],
        out_specs=pl.BlockSpec(memory_space=pltpu.VMEM),
        scratch_shapes=[
            pltpu.VMEM((B, 512), BF16),
            pltpu.VMEM((LAYERS, 512), BF16),
            pltpu.VMEM((LAYERS, 512, 10 * HD), BF16),
            pltpu.VMEM((LAYERS, 8 * HD, 512), BF16),
            pltpu.VMEM((LAYERS, B, SEG, HD), BF16),
            pltpu.VMEM((LAYERS, B, SEG, HD), BF16),
            pltpu.VMEM((B, HD), F32),
            pltpu.VMEM((1, 8, B, PART), F32),
            pltpu.VMEM((1, 8, 3, B, PART), F32),
            pltpu.VMEM((LAYERS, 8, B, 512), F32),
            pltpu.VMEM((LAYERS, HD, B * SEG), BF16),
            pltpu.VMEM((LAYERS - 1, B, 2, SEG, HD), F32),
            pltpu.VMEM((LAYERS - 1, B, 2, SEG, HD), F32),
            pltpu.VMEM((LAYERS - 1, B * SEG, HD), BF16),
            pltpu.VMEM((LAYERS - 1, B * 16, HD), F32),
            pltpu.VMEM((LAYERS - 1, 15, 16, HD), F32),
            pltpu.VMEM((LAYERS - 1, 16 * 16, HD), F32),
            pltpu.SemaphoreType.DMA((LAYERS, 6)),
            pltpu.SemaphoreType.DMA((3,)),
            pltpu.SemaphoreType.DMA((1, 8, 3)),
            pltpu.SemaphoreType.DMA((1, 8, 3)),
            pltpu.SemaphoreType.DMA((LAYERS, 7)),
            pltpu.SemaphoreType.DMA((LAYERS, 7)),
            pltpu.SemaphoreType.DMA((LAYERS - 1, 7)),
            pltpu.SemaphoreType.DMA((LAYERS - 1, 7)),
            pltpu.SemaphoreType.DMA((LAYERS - 1, 15)),
            pltpu.SemaphoreType.DMA((LAYERS - 1, 15)),
            pltpu.SemaphoreType.DMA((LAYERS - 1, 15)),
            pltpu.SemaphoreType.DMA((LAYERS - 1, 15)),
        ],
        compiler_params=pltpu.CompilerParams(
            collective_id=0, has_side_effects=True, vmem_limit_bytes=60 * 1024 * 1024
        ),
    )(hidden, norm_gains, w_query, w_key, w_value, w_out, key_cache, value_cache, lengths, freq)


def solution(mesh):
    return jax.shard_map(
        on_device,
        mesh=mesh,
        in_specs=(
            P(None, "ctx"),
            P(None, "ctx"),
            P(None, "ctx", "tp"),
            P(None, "ctx", "tp"),
            P(None, "ctx", "tp"),
            P(None, "tp", "ctx"),
            P(None, None, "tp", "ctx", None),
            P(None, None, "tp", "ctx", None),
            P(),
        ),
        out_specs=P(None, "ctx"),
        check_vma=False,
    )
```

```python
import functools
import math

import jax
import jax.numpy as jnp
import numpy as np
from jax import lax
from jax.experimental import pallas as pl
from jax.experimental.pallas import tpu as pltpu
from jax.sharding import PartitionSpec as P

MESH = pl.DeviceIdType.MESH
LAYERS = 4
B = 8
HD = 128
HALF = 64
D = 8192
SEG = 128
FILL = -1e30
EPS = 1e-5
ROPE_BASE = 500000.0
F32 = jnp.float32
BF16 = jnp.bfloat16
QA = 5 * HD
QB = 5 * HD
PART = 6 * HD
PLANE_ORDER = (10, 6, 9, 11, 14, 2, 8, 5, 7, 13, 15, 1, 3, 4, 12)
UNIT = 32
SHIFTS = ((1, 0), (2, 0), (3, 0), (0, 1), (1, 1), (2, 1), (3, 1))
NEAR, FAR = (1, 3, 0, 2), (5, 4, 6)
PLAN = (
    (2, 2, 2, 2, 3, 2, 2, 3, 2, 2, 2, 0, 0, 0),
    (0, 0, 3, 3, 3, 3, 2, 3, 2, 2, 3, 0, 0, 0),
)


def tile(value, i):
    return value[:, i * HD : (i + 1) * HD]


def add_up(terms):
    while len(terms) > 1:
        pairs = [terms[i] + terms[i + 1] for i in range(0, len(terms) - 1, 2)]
        terms = pairs + terms[len(terms) - len(terms) % 2 :]
    return terms[0]


def kernel(
    hidden, gains, w_query, w_key, w_value, w_out, key_cache, value_cache, lengths, freq,
    out,
    hbuf, gbuf, wqkv, wo, kbuf, vbuf, fbuf, snd, rcv, tpb, keys_t, stage, moved, values, qsnd, qrcv, orcv,
    lsem, psem, ssem, rsem, tssem, trsem, bssem, brsem, qssem, qrsem, ossem, orsem,
):
    c = lax.axis_index("ctx")
    t = lax.axis_index("tp")
    y, x = c // 4, lax.rem(c, 4)
    core = lax.rem(t, 2)

    def seat(y, x):
        u, v = x + core * (y - x), y + core * (x - y)
        return v // 2, lax.rem(v, 2) * 4 + u

    def place(part, sequence):
        u, v = lax.rem(sequence, 4), part * 2 + sequence // 4
        return (v + core * (u - v)) * 4 + u + core * (v - u)

    part, mine = seat(y, x)
    seat_index = part * 8 + mine

    def weight_loads(l):
        return (
            pltpu.make_async_copy(w_query.at[l], wqkv.at[l, :, pl.ds(0, 8 * HD)], lsem.at[l, 0]),
            pltpu.make_async_copy(w_key.at[l], wqkv.at[l, :, pl.ds(8 * HD, HD)], lsem.at[l, 1]),
            pltpu.make_async_copy(w_value.at[l], wqkv.at[l, :, pl.ds(9 * HD, HD)], lsem.at[l, 2]),
            pltpu.make_async_copy(key_cache.at[l, :, 0], kbuf.at[l], lsem.at[l, 3]),
            pltpu.make_async_copy(value_cache.at[l, :, 0], vbuf.at[l], lsem.at[l, 4]),
            pltpu.make_async_copy(w_out.at[l], wo.at[l], lsem.at[l, 5]),
        )

    small = (
        pltpu.make_async_copy(hidden, hbuf, psem.at[0]),
        pltpu.make_async_copy(gains, gbuf, psem.at[1]),
        pltpu.make_async_copy(freq, fbuf, psem.at[2]),
    )
    along_x = [(y * 4 + lax.rem(x + d, 4), t) for d in (1, 2, 3)]
    along_y = [(lax.rem(y + d, 4) * 4 + x, t) for d in (1, 2, 3)]
    along_t = [(c, lax.rem(t + d, 8)) for d in range(1, 8)]
    plane = [(lax.rem(y + d // 4, 4) * 4 + lax.rem(x + d % 4, 4), t) for d in range(1, 16)]
    barrier = pltpu.get_barrier_semaphore()
    for peer in along_x + along_y + along_t:
        pl.semaphore_signal(barrier, inc=1, device_id=peer, device_id_type=MESH)
    for copy in small:
        copy.start()
    loads = [weight_loads(l) for l in range(LAYERS)]
    for copy in loads[0][:3]:
        copy.start()

    lane = lax.broadcasted_iota(jnp.int32, (B, HD), 1)
    row = lax.broadcasted_iota(jnp.int32, (B, HD), 0)
    length = jnp.zeros((B, HD), jnp.int32)
    for b in range(B):
        length = jnp.where(row == b, lengths[b], length)
    usable = c * SEG + lane < length
    my_length = lengths[mine]
    small[2].wait()

    def angles(positions):
        angle = positions.astype(F32) * fbuf[...]
        sine = jnp.sin(angle)
        return jnp.cos(angle), jnp.where(lane < HALF, -sine, sine)

    cosine, sine = angles(length)
    my_cosine, my_sine = angles(jnp.full((B, HD), my_length, jnp.int32))
    small[0].wait()
    small[1].wait()
    stream = hbuf[...].astype(F32)

    def exchange(l, phase, width, peers):
        copies = []
        for i in (1, 0, 2):
            copy = pltpu.make_async_remote_copy(
                src_ref=snd.at[l, phase, :, pl.ds(0, width)],
                dst_ref=rcv.at[l, phase, i, :, pl.ds(0, width)],
                send_sem=ssem.at[l, phase, i],
                recv_sem=rsem.at[l, phase, i],
                device_id=peers[i],
                device_id_type=MESH,
            )
            copy.start()
            copies.append(copy)
        return copies

    def arrive(copies):
        for copy in copies:
            copy.wait_recv()

    def total(l, phase, width):
        own = snd[l, phase, :, :width]
        got = [rcv[l, phase, i, :, :width] for i in range(3)]
        return (own + got[0]) + (got[1] + got[2])

    def merge(l, phase, fresh=None):
        outs = [snd[l, phase, :, : 4 * HD]] + [rcv[l, phase, i, :, : 4 * HD] for i in range(3)]
        stats = [snd[l, phase, :, 4 * HD : 5 * HD]] + [
            rcv[l, phase, i, :, 4 * HD : 5 * HD] for i in range(3)
        ]
        sums = [pltpu.roll(s, HALF, 1) for s in stats]
        top = jnp.maximum(jnp.maximum(stats[0], stats[1]), jnp.maximum(stats[2], stats[3]))
        if fresh is not None:
            top = jnp.maximum(top, fresh[0])
        scale = [jnp.exp(s - top) for s in stats]
        whole = (scale[0] * sums[0] + scale[1] * sums[1]) + (scale[2] * sums[2] + scale[3] * sums[3])
        if fresh is not None:
            new = jnp.exp(fresh[0] - top)
            whole = whole + new
            scale = [s / whole for s in scale]
            new = new.astype(BF16).astype(F32) / whole
        result = []
        for j in range(4):
            parts = [jnp.broadcast_to(s[:, j : j + 1], (B, HD)) * tile(o, j) for s, o in zip(scale, outs)]
            joined = (parts[0] + parts[1]) + (parts[2] + parts[3])
            if fresh is not None:
                joined = joined + jnp.broadcast_to(new[:, j : j + 1], (B, HD)) * fresh[1]
            result.append(joined)
        return result, top, whole


    def widen(l):
        loads[l][3].wait()
        loads[l][4].wait()
        for b in range(B):
            stage[l - 1, b, 0] = kbuf[l, b].astype(F32)
            stage[l - 1, b, 1] = vbuf[l, b].astype(F32)
        moved[l - 1, mine, 0] = stage[l - 1, mine, 0]
        moved[l - 1, mine, 1] = stage[l - 1, mine, 1]

    def shifted(dx, other, sign=1):
        return lax.rem(mine // 4 + other, 2) * 4 + lax.rem(lax.rem(mine, 4) + 4 + sign * dx, 4)

    def moved_copy(l, j, to, src, dst):
        return pltpu.make_async_remote_copy(
            src_ref=src,
            dst_ref=dst,
            send_sem=bssem.at[l - 1, j],
            recv_sem=brsem.at[l - 1, j],
            device_id=(place(part, to), t),
            device_id_type=MESH,
        )

    def move(l, unit, group):
        which, rows = unit // (SEG // UNIT), pl.ds(unit % (SEG // UNIT) * UNIT, UNIT)
        for j in group:
            to = shifted(*SHIFTS[j])
            moved_copy(
                l, j, to, stage.at[l - 1, to, which, rows], moved.at[l - 1, mine, which, rows]
            ).start()

    def moves(l):
        result = []
        for j in range(7):
            to, origin = shifted(*SHIFTS[j]), shifted(*SHIFTS[j], sign=-1)
            result.append(moved_copy(l, j, to, stage.at[l - 1, to], moved.at[l - 1, origin]))
        return result

    def narrow(l):
        for queue, group in ((near, NEAR), (far, FAR)):
            units(queue, sum(item[0] <= l for item in queue), group)
        arrive(moves(l))
        for s in range(8):
            keys_t[l, :, s * SEG : (s + 1) * SEG] = moved[l - 1, s, 0].T.astype(BF16)
            values[l - 1, s * SEG : (s + 1) * SEG] = moved[l - 1, s, 1].astype(BF16)

    widened = []

    def units(queue, count, group):
        for _ in range(min(count, len(queue))):
            l, u = queue.pop(0)
            if l not in widened:
                widened.append(l)
                widen(l)
            move(l, u, group)

    every = [(l, u) for l in range(1, LAYERS) for u in range(2 * SEG // UNIT)]
    near, far = list(every), list(every)

    def background():
        units(near, PLAN[0][len(steps)], NEAR)
        units(far, PLAN[1][len(steps)], FAR)
        steps.append(1)

    steps = []
    sent = []

    held = jnp.concatenate([place(part, s) * SEG + lane for s in range(B)], axis=1)
    within = held < my_length

    def first_layer(l, load, scaled, squares):
        nonlocal sent
        snd[l, 0, :, :QA] = jnp.dot(scaled, wqkv[l, :, :QA], preferred_element_type=F32)
        snd[l, 0, :, QA : QA + HD] = squares
        snd[l, 1, :, :QB] = jnp.dot(scaled, wqkv[l, :, QA:], preferred_element_type=F32)
        pl.semaphore_wait(barrier, 13)
        a1 = exchange(l, 0, QA + HD, along_x)
        b1 = exchange(l, 1, QB, along_y)
        for copy in loads[0][3:]:
            copy.start()
        for group in loads[1:]:
            for copy in group:
                copy.start()
        load[3].wait()
        load[4].wait()
        for b in range(B):
            keys_t[0, :, b * SEG : (b + 1) * SEG] = kbuf[0, b].astype(F32).T.astype(BF16)
        background()
        arrive(a1)
        snd[l, 2, :, : QA + HD] = total(l, 0, QA + HD)
        a2 = exchange(l, 2, QA + HD, along_y)
        arrive(b1)
        snd[l, 3, :, :QB] = total(l, 1, QB)
        b2 = exchange(l, 3, QB, along_x)
        background()
        arrive(a2)
        first = total(l, 2, QA + HD)
        inverse = lax.rsqrt(jnp.sum(tile(first, 5), axis=1, keepdims=True) / D + EPS)
        cos_l, sin_l = cosine * inverse, sine * inverse

        def rotate(u):
            return u * cos_l + pltpu.roll(u, HALF, 1) * sin_l

        arrive(b2)
        second = total(l, 3, QB)
        raw = [tile(first, i) for i in range(5)] + [tile(second, i) for i in range(3)]
        query = jnp.concatenate([rotate(u) for u in raw], axis=0).astype(BF16)
        new_key = rotate(tile(second, 3)).astype(BF16).astype(F32)
        new_value = (tile(second, 4) * inverse).astype(BF16).astype(F32)

        score = jnp.dot(query, keys_t[l], preferred_element_type=F32)
        probs, tops, sums = [], [], []
        for h in range(8):
            block = score[h * B : (h + 1) * B]
            s = tile(block, 0)
            for b in range(1, B):
                s = jnp.where(row == b, tile(block, b), s)
            s = jnp.where(usable, s * (1.0 / math.sqrt(HD)), FILL)
            top = jnp.max(s, axis=1, keepdims=True)
            p = jnp.where(usable, jnp.exp(s - top), 0.0)
            tops.append(top)
            sums.append(jnp.sum(p, axis=1, keepdims=True))
            probs.append(jnp.concatenate([jnp.where(row == b, p, 0.0) for b in range(B)], axis=1))
        probs = jnp.concatenate(probs, axis=0).astype(BF16)
        mixed = jnp.dot(probs, vbuf[l].reshape(B * SEG, HD), preferred_element_type=F32)

        def store_half(phase, start):
            stats = jnp.zeros((B, HD), F32)
            for j in range(4):
                h = start + j
                snd[l, phase, :, j * HD : (j + 1) * HD] = mixed[h * B : (h + 1) * B]
                stats = jnp.where(lane == j, tops[h], stats)
                stats = jnp.where(lane == HALF + j, sums[h], stats)
            snd[l, phase, :, 4 * HD : 5 * HD] = stats

        store_half(4, 0)
        a3 = exchange(l, 4, 5 * HD, along_x)
        store_half(5, 4)
        b3 = exchange(l, 5, 5 * HD, along_y)
        background()
        own = [jnp.zeros((B, HD), F32), jnp.zeros((B, HD), F32)]
        for h in range(8):
            dot = jnp.sum(query[h * B : (h + 1) * B].astype(F32) * new_key, axis=1, keepdims=True)
            own[h // 4] = jnp.where(lane == h % 4, dot * (1.0 / math.sqrt(HD)), own[h // 4])

        def pass_on(phase_in, phase_out):
            joined, top, whole = merge(l, phase_in)
            for j in range(4):
                snd[l, phase_out, :, j * HD : (j + 1) * HD] = joined[j]
            snd[l, phase_out, :, 4 * HD : 5 * HD] = jnp.where(lane < HALF, top, pltpu.roll(whole, HALF, 1))

        arrive(a3)
        pass_on(4, 6)
        a4 = exchange(l, 6, 5 * HD, along_y)
        arrive(b3)
        pass_on(5, 7)
        b4 = exchange(l, 7, 5 * HD, along_x)
        background()
        load[5].wait()
        arrive(a4)
        context = jnp.concatenate(merge(l, 6, (own[0], new_value))[0], axis=1).astype(BF16)
        head_part = jnp.dot(context, wo[l, : 4 * HD, :], preferred_element_type=F32)
        arrive(b4)
        context = jnp.concatenate(merge(l, 7, (own[1], new_value))[0], axis=1).astype(BF16)
        head_part = head_part + jnp.dot(context, wo[l, 4 * HD :, :], preferred_element_type=F32)
        sent += a1 + b1 + a2 + b2 + a3 + b3 + a4 + b4
        return head_part

    def later_layer(l, load, scaled, squares):
        nonlocal sent

        raw = jnp.dot(scaled, wqkv[l], preferred_element_type=F32)
        for i in range(10):
            qsnd[l - 1, pl.ds(i, B, stride=16), :] = tile(raw, i)
        qsnd[l - 1, pl.ds(10, B, stride=16), :] = squares
        copies = []
        for d in PLANE_ORDER:
            to = plane[d - 1]
            rows = pl.ds(pl.multiple_of(seat(to[0] // 4, lax.rem(to[0], 4))[1] * 16, 16), 11)
            copy = pltpu.make_async_remote_copy(
                src_ref=qsnd.at[l - 1, rows],
                dst_ref=qrcv.at[l - 1, d - 1, pl.ds(0, 11)],
                send_sem=qssem.at[l - 1, d - 1],
                recv_sem=qrsem.at[l - 1, d - 1],
                device_id=to,
                device_id_type=MESH,
            )
            copy.start()
            copies.append(copy)
        sent += copies
        background()
        narrow(l)
        at = pl.multiple_of(mine * 16, 16)
        heads = [qsnd[l - 1, pl.ds(at, 8), :]]
        others = [qsnd[l - 1, pl.ds(at + 8, 3), :]]
        arrive(copies)
        for d in range(15):
            heads.append(qrcv[l - 1, d, 0:8, :])
            others.append(qrcv[l - 1, d, 8:11, :])
        heads, others = add_up(heads), add_up(others)
        inverse = lax.rsqrt(jnp.sum(others[2:3], axis=1, keepdims=True) / D + EPS)

        def rotate(u, rows):
            u = u * inverse
            return u * my_cosine[:rows] + pltpu.roll(u, HALF, 1) * my_sine[:rows]

        query = rotate(heads, 8).astype(BF16)
        new_key = rotate(jnp.broadcast_to(others[0:1], (B, HD)), 8).astype(BF16).astype(F32)
        new_value = (others[1:2] * inverse).astype(BF16).astype(F32)
        scale = 1.0 / math.sqrt(HD)
        score = jnp.dot(query, keys_t[l], preferred_element_type=F32)
        own = jnp.sum(query.astype(F32) * new_key, axis=1, keepdims=True) * scale
        own = jnp.where(part == 0, own, FILL)
        score = jnp.where(within, score * scale, FILL)
        top = jnp.maximum(jnp.max(score, axis=1, keepdims=True), own)
        p = jnp.where(within, jnp.exp(score - top), 0.0)
        fresh = jnp.where(part == 0, jnp.exp(own - top), 0.0)
        weight = jnp.sum(p, axis=1, keepdims=True) + fresh
        mixed = jnp.dot(p.astype(BF16), values[l - 1], preferred_element_type=F32)
        mixed = mixed + fresh.astype(BF16).astype(F32) * new_value
        stats = jnp.where(lane == row, top, 0.0) + jnp.where(lane == row + HALF, weight, 0.0)
        base = pl.multiple_of(seat_index * 16, 16)
        orcv[l - 1, pl.ds(base, 8), :] = mixed
        orcv[l - 1, pl.ds(base + 8, 1), :] = jnp.sum(stats, axis=0, keepdims=True)
        copies = []
        for d in PLANE_ORDER:
            copy = pltpu.make_async_remote_copy(
                src_ref=orcv.at[l - 1, pl.ds(base, 9)],
                dst_ref=orcv.at[l - 1, pl.ds(base, 9)],
                send_sem=ossem.at[l - 1, d - 1],
                recv_sem=orsem.at[l - 1, d - 1],
                device_id=plane[d - 1],
                device_id_type=MESH,
            )
            copy.start()
            copies.append(copy)
        sent += copies
        background()
        load[5].wait()
        arrive(copies)
        low = orcv[l - 1, pl.ds(8, B, stride=16), :]
        high = orcv[l - 1, pl.ds(128 + 8, B, stride=16), :]
        top = jnp.maximum(low, high)
        scales = [jnp.exp(low - top), jnp.exp(high - top)]
        whole = scales[0] * pltpu.roll(low, HALF, 1) + scales[1] * pltpu.roll(high, HALF, 1)
        scales = [s / whole for s in scales]
        context = []
        for h in range(8):
            context.append(
                jnp.broadcast_to(scales[0][:, h : h + 1], (B, HD)) * orcv[l - 1, pl.ds(h, B, stride=16), :]
                + jnp.broadcast_to(scales[1][:, h : h + 1], (B, HD)) * orcv[l - 1, pl.ds(128 + h, B, stride=16), :]
            )
        context = jnp.concatenate(context, axis=1).astype(BF16)
        return jnp.dot(context, wo[l], preferred_element_type=F32)

    for l in range(LAYERS):
        load = loads[l]
        gain = gbuf[l : l + 1, :].astype(F32)
        scaled = (stream * gain).astype(BF16)
        squares = stream * stream
        squares = (tile(squares, 0) + tile(squares, 1)) + (tile(squares, 2) + tile(squares, 3))
        for i in range(3):
            load[i].wait()
        head_part = (first_layer if l == 0 else later_layer)(l, load, scaled, squares)

        tpb[l, t] = head_part
        copies = []
        for d in (4, 5, 3, 2, 6, 1, 7):
            copy = pltpu.make_async_remote_copy(
                src_ref=tpb.at[l, t],
                dst_ref=tpb.at[l, t],
                send_sem=tssem.at[l, d - 1],
                recv_sem=trsem.at[l, d - 1],
                device_id=along_t[d - 1],
                device_id_type=MESH,
            )
            copy.start()
            copies.append(copy)
        sent += copies
        background()
        arrive(copies)
        stream = stream + add_up([tpb[l, i] for i in range(8)])
    out[...] = stream
    for l in range(1, LAYERS):
        sent += moves(l)
    for copy in sent:
        copy.wait_send()


def on_device(hidden, norm_gains, w_query, w_key, w_value, w_out, key_cache, value_cache, lengths):
    exponents = np.arange(HALF, dtype=np.float32) * np.float32(2.0 / HD)
    freq = np.exp(-exponents.astype(np.float64) * math.log(ROPE_BASE)).astype(np.float32)
    freq = jnp.asarray(np.tile(np.concatenate([freq, freq])[None, :], (B, 1)))
    hbm = pl.BlockSpec(memory_space=pl.ANY)
    return pl.pallas_call(
        kernel,
        out_shape=jax.ShapeDtypeStruct((B, 512), F32),
        in_specs=[hbm] * 8 + [pl.BlockSpec(memory_space=pltpu.SMEM), hbm],
        out_specs=pl.BlockSpec(memory_space=pltpu.VMEM),
        scratch_shapes=[
            pltpu.VMEM((B, 512), BF16),
            pltpu.VMEM((LAYERS, 512), BF16),
            pltpu.VMEM((LAYERS, 512, 10 * HD), BF16),
            pltpu.VMEM((LAYERS, 8 * HD, 512), BF16),
            pltpu.VMEM((LAYERS, B, SEG, HD), BF16),
            pltpu.VMEM((LAYERS, B, SEG, HD), BF16),
            pltpu.VMEM((B, HD), F32),
            pltpu.VMEM((1, 8, B, PART), F32),
            pltpu.VMEM((1, 8, 3, B, PART), F32),
            pltpu.VMEM((LAYERS, 8, B, 512), F32),
            pltpu.VMEM((LAYERS, HD, B * SEG), BF16),
            pltpu.VMEM((LAYERS - 1, B, 2, SEG, HD), F32),
            pltpu.VMEM((LAYERS - 1, B, 2, SEG, HD), F32),
            pltpu.VMEM((LAYERS - 1, B * SEG, HD), BF16),
            pltpu.VMEM((LAYERS - 1, B * 16, HD), F32),
            pltpu.VMEM((LAYERS - 1, 15, 16, HD), F32),
            pltpu.VMEM((LAYERS - 1, 16 * 16, HD), F32),
            pltpu.SemaphoreType.DMA((LAYERS, 6)),
            pltpu.SemaphoreType.DMA((3,)),
            pltpu.SemaphoreType.DMA((1, 8, 3)),
            pltpu.SemaphoreType.DMA((1, 8, 3)),
            pltpu.SemaphoreType.DMA((LAYERS, 7)),
            pltpu.SemaphoreType.DMA((LAYERS, 7)),
            pltpu.SemaphoreType.DMA((LAYERS - 1, 7)),
            pltpu.SemaphoreType.DMA((LAYERS - 1, 7)),
            pltpu.SemaphoreType.DMA((LAYERS - 1, 15)),
            pltpu.SemaphoreType.DMA((LAYERS - 1, 15)),
            pltpu.SemaphoreType.DMA((LAYERS - 1, 15)),
            pltpu.SemaphoreType.DMA((LAYERS - 1, 15)),
        ],
        compiler_params=pltpu.CompilerParams(
            collective_id=0, has_side_effects=True, vmem_limit_bytes=60 * 1024 * 1024
        ),
    )(hidden, norm_gains, w_query, w_key, w_value, w_out, key_cache, value_cache, lengths, freq)


def solution(mesh):
    return jax.shard_map(
        on_device,
        mesh=mesh,
        in_specs=(
            P(None, "ctx"),
            P(None, "ctx"),
            P(None, "ctx", "tp"),
            P(None, "ctx", "tp"),
            P(None, "ctx", "tp"),
            P(None, "tp", "ctx"),
            P(None, None, "tp", "ctx", None),
            P(None, None, "tp", "ctx", None),
            P(),
        ),
        out_specs=P(None, "ctx"),
        check_vma=False,
    )
```

```python
import functools
import math

import jax
import jax.numpy as jnp
import numpy as np
from jax import lax
from jax.experimental import pallas as pl
from jax.experimental.pallas import tpu as pltpu
from jax.sharding import PartitionSpec as P

MESH = pl.DeviceIdType.MESH
LAYERS = 4
B = 8
HD = 128
HALF = 64
D = 8192
SEG = 128
FILL = -1e30
EPS = 1e-5
ROPE_BASE = 500000.0
F32 = jnp.float32
BF16 = jnp.bfloat16
QA = 5 * HD
QB = 5 * HD
PART = 6 * HD
PLANE_ORDER = (10, 6, 9, 11, 14, 2, 8, 5, 7, 13, 15, 1, 3, 4, 12)
UNIT = 32
SHIFTS = ((1, 0), (2, 0), (3, 0), (0, 1), (1, 1), (2, 1), (3, 1))
NEAR, FAR = (1, 3, 0, 2), (5, 4, 6)
PLAN = (
    (2, 1, 2, 2, 3, 3, 3, 3, 2, 2, 1, 0, 0, 0),
    (0, 0, 2, 3, 4, 3, 3, 3, 2, 2, 2, 0, 0, 0),
)


def tile(value, i):
    return value[:, i * HD : (i + 1) * HD]


def add_up(terms):
    while len(terms) > 1:
        pairs = [terms[i] + terms[i + 1] for i in range(0, len(terms) - 1, 2)]
        terms = pairs + terms[len(terms) - len(terms) % 2 :]
    return terms[0]


def kernel(
    hidden, gains, w_query, w_key, w_value, w_out, key_cache, value_cache, lengths_in, freq,
    out,
    hbuf, gbuf, wqkv, wo, kbuf, vbuf, fbuf, snd, rcv, tpb, keys_t, stage, moved, values, qsnd, qrcv, orcv, obuf, lengths,
    lsem, psem, ssem, rsem, tssem, trsem, bssem, brsem, qssem, qrsem, ossem, orsem,
):
    c = lax.axis_index("ctx")
    t = lax.axis_index("tp")
    y, x = c // 4, lax.rem(c, 4)
    core = lax.rem(t, 2)

    def seat(y, x):
        u, v = x + core * (y - x), y + core * (x - y)
        return v // 2, lax.rem(v, 2) * 4 + u

    def place(part, sequence):
        u, v = lax.rem(sequence, 4), part * 2 + sequence // 4
        return (v + core * (u - v)) * 4 + u + core * (v - u)

    part, mine = seat(y, x)
    seat_index = part * 8 + mine

    def weight_loads(l):
        return (
            pltpu.make_async_copy(w_query.at[l], wqkv.at[l, :, pl.ds(0, 8 * HD)], lsem.at[l, 0]),
            pltpu.make_async_copy(w_key.at[l], wqkv.at[l, :, pl.ds(8 * HD, HD)], lsem.at[l, 1]),
            pltpu.make_async_copy(w_value.at[l], wqkv.at[l, :, pl.ds(9 * HD, HD)], lsem.at[l, 2]),
            pltpu.make_async_copy(key_cache.at[l, :, 0], kbuf.at[l], lsem.at[l, 3]),
            pltpu.make_async_copy(value_cache.at[l, :, 0], vbuf.at[l], lsem.at[l, 4]),
            pltpu.make_async_copy(w_out.at[l], wo.at[l], lsem.at[l, 5]),
        )

    small = (
        pltpu.make_async_copy(hidden, hbuf, psem.at[0]),
        pltpu.make_async_copy(gains, gbuf, psem.at[1]),
        pltpu.make_async_copy(freq, fbuf, psem.at[2]),
        pltpu.make_async_copy(lengths_in, lengths, psem.at[3]),
    )
    along_x = [(y * 4 + lax.rem(x + d, 4), t) for d in (1, 2, 3)]
    along_y = [(lax.rem(y + d, 4) * 4 + x, t) for d in (1, 2, 3)]
    along_t = [(c, lax.rem(t + d, 8)) for d in range(1, 8)]
    plane = [(lax.rem(y + d // 4, 4) * 4 + lax.rem(x + d % 4, 4), t) for d in range(1, 16)]
    barrier = pltpu.get_barrier_semaphore()
    for peer in along_x + along_y + along_t:
        pl.semaphore_signal(barrier, inc=1, device_id=peer, device_id_type=MESH)
    for copy in small:
        copy.start()
    loads = [weight_loads(l) for l in range(LAYERS)]
    for copy in loads[0][:3]:
        copy.start()

    lane = lax.broadcasted_iota(jnp.int32, (B, HD), 1)
    row = lax.broadcasted_iota(jnp.int32, (B, HD), 0)
    def positions():
        small[3].wait()
        length = jnp.zeros((B, HD), jnp.int32)
        for b in range(B):
            length = jnp.where(row == b, lengths[b], length)
        usable = c * SEG + lane < length
        my_length = lengths[mine]
        small[2].wait()

        def angles(positions):
            angle = positions.astype(F32) * fbuf[...]
            sine = jnp.sin(angle)
            return jnp.cos(angle), jnp.where(lane < HALF, -sine, sine)

        cosine, sine = angles(length)
        my_cosine, my_sine = angles(jnp.full((B, HD), my_length, jnp.int32))
        held = jnp.concatenate([place(part, s) * SEG + lane for s in range(B)], axis=1)
        within = held < my_length
        return usable, cosine, sine, my_cosine, my_sine, within

    small[0].wait()
    small[1].wait()
    stream = hbuf[...].astype(F32)

    def exchange(l, phase, width, peers):
        copies = []
        for i in (1, 0, 2):
            copy = pltpu.make_async_remote_copy(
                src_ref=snd.at[l, phase, :, pl.ds(0, width)],
                dst_ref=rcv.at[l, phase, i, :, pl.ds(0, width)],
                send_sem=ssem.at[l, phase, i],
                recv_sem=rsem.at[l, phase, i],
                device_id=peers[i],
                device_id_type=MESH,
            )
            copy.start()
            copies.append(copy)
        return copies

    def arrive(copies):
        for copy in copies:
            copy.wait_recv()

    def total(l, phase, width):
        own = snd[l, phase, :, :width]
        got = [rcv[l, phase, i, :, :width] for i in range(3)]
        return (own + got[0]) + (got[1] + got[2])

    def merge(l, phase, fresh=None):
        outs = [snd[l, phase, :, : 4 * HD]] + [rcv[l, phase, i, :, : 4 * HD] for i in range(3)]
        stats = [snd[l, phase, :, 4 * HD : 5 * HD]] + [
            rcv[l, phase, i, :, 4 * HD : 5 * HD] for i in range(3)
        ]
        sums = [pltpu.roll(s, HALF, 1) for s in stats]
        top = jnp.maximum(jnp.maximum(stats[0], stats[1]), jnp.maximum(stats[2], stats[3]))
        if fresh is not None:
            top = jnp.maximum(top, fresh[0])
        scale = [jnp.exp(s - top) for s in stats]
        whole = (scale[0] * sums[0] + scale[1] * sums[1]) + (scale[2] * sums[2] + scale[3] * sums[3])
        if fresh is not None:
            new = jnp.exp(fresh[0] - top)
            whole = whole + new
            scale = [s / whole for s in scale]
            new = new.astype(BF16).astype(F32) / whole
        result = []
        for j in range(4):
            parts = [jnp.broadcast_to(s[:, j : j + 1], (B, HD)) * tile(o, j) for s, o in zip(scale, outs)]
            joined = (parts[0] + parts[1]) + (parts[2] + parts[3])
            if fresh is not None:
                joined = joined + jnp.broadcast_to(new[:, j : j + 1], (B, HD)) * fresh[1]
            result.append(joined)
        return result, top, whole


    def widen(l):
        loads[l][3].wait()
        loads[l][4].wait()
        for b in range(B):
            stage[l - 1, b, 0] = kbuf[l, b].astype(F32)
            stage[l - 1, b, 1] = vbuf[l, b].astype(F32)
        moved[l - 1, mine, 0] = stage[l - 1, mine, 0]
        moved[l - 1, mine, 1] = stage[l - 1, mine, 1]

    def shifted(dx, other, sign=1):
        return lax.rem(mine // 4 + other, 2) * 4 + lax.rem(lax.rem(mine, 4) + 4 + sign * dx, 4)

    def moved_copy(l, j, to, src, dst):
        return pltpu.make_async_remote_copy(
            src_ref=src,
            dst_ref=dst,
            send_sem=bssem.at[l - 1, j],
            recv_sem=brsem.at[l - 1, j],
            device_id=(place(part, to), t),
            device_id_type=MESH,
        )

    def move(l, unit, group):
        which, rows = unit // (SEG // UNIT), pl.ds(unit % (SEG // UNIT) * UNIT, UNIT)
        for j in group:
            to = shifted(*SHIFTS[j])
            moved_copy(
                l, j, to, stage.at[l - 1, to, which, rows], moved.at[l - 1, mine, which, rows]
            ).start()

    def moves(l):
        result = []
        for j in range(7):
            to, origin = shifted(*SHIFTS[j]), shifted(*SHIFTS[j], sign=-1)
            result.append(moved_copy(l, j, to, stage.at[l - 1, to], moved.at[l - 1, origin]))
        return result

    def narrow(l):
        for queue, group in ((near, NEAR), (far, FAR)):
            units(queue, sum(item[0] <= l for item in queue), group)
        arrive(moves(l))
        for s in range(8):
            keys_t[l, :, s * SEG : (s + 1) * SEG] = moved[l - 1, s, 0].T.astype(BF16)
            values[l - 1, s * SEG : (s + 1) * SEG] = moved[l - 1, s, 1].astype(BF16)

    widened = []

    def units(queue, count, group):
        for _ in range(min(count, len(queue))):
            l, u = queue.pop(0)
            if l not in widened:
                widened.append(l)
                widen(l)
            move(l, u, group)

    every = [(l, u) for l in range(1, LAYERS) for u in range(2 * SEG // UNIT)]
    near, far = list(every), list(every)

    def background():
        units(near, PLAN[0][len(steps)], NEAR)
        units(far, PLAN[1][len(steps)], FAR)
        steps.append(1)

    steps = []
    shared = []
    sent = []

    def first_layer(l, load, scaled, squares):
        nonlocal sent
        snd[l, 0, :, :QA] = jnp.dot(scaled, wqkv[l, :, :QA], preferred_element_type=F32)
        snd[l, 0, :, QA : QA + HD] = squares
        snd[l, 1, :, :QB] = jnp.dot(scaled, wqkv[l, :, QA:], preferred_element_type=F32)
        pl.semaphore_wait(barrier, 13)
        a1 = exchange(l, 0, QA + HD, along_x)
        b1 = exchange(l, 1, QB, along_y)
        for copy in loads[0][3:]:
            copy.start()
        for group in loads[1:]:
            for copy in group:
                copy.start()
        usable, cosine, sine, my_cosine, my_sine, within = known = positions()
        shared.extend(known[3:])
        load[3].wait()
        load[4].wait()
        for b in range(B):
            keys_t[0, :, b * SEG : (b + 1) * SEG] = kbuf[0, b].astype(F32).T.astype(BF16)
        background()
        arrive(a1)
        snd[l, 2, :, : QA + HD] = total(l, 0, QA + HD)
        a2 = exchange(l, 2, QA + HD, along_y)
        arrive(b1)
        snd[l, 3, :, :QB] = total(l, 1, QB)
        b2 = exchange(l, 3, QB, along_x)
        background()
        arrive(a2)
        first = total(l, 2, QA + HD)
        inverse = lax.rsqrt(jnp.sum(tile(first, 5), axis=1, keepdims=True) / D + EPS)
        cos_l, sin_l = cosine * inverse, sine * inverse

        def rotate(u):
            return u * cos_l + pltpu.roll(u, HALF, 1) * sin_l

        arrive(b2)
        second = total(l, 3, QB)
        raw = [tile(first, i) for i in range(5)] + [tile(second, i) for i in range(3)]
        query = jnp.concatenate([rotate(u) for u in raw], axis=0).astype(BF16)
        new_key = rotate(tile(second, 3)).astype(BF16).astype(F32)
        new_value = (tile(second, 4) * inverse).astype(BF16).astype(F32)

        score = jnp.dot(query, keys_t[l], preferred_element_type=F32)
        probs, tops, sums = [], [], []
        for h in range(8):
            block = score[h * B : (h + 1) * B]
            s = tile(block, 0)
            for b in range(1, B):
                s = jnp.where(row == b, tile(block, b), s)
            s = jnp.where(usable, s * (1.0 / math.sqrt(HD)), FILL)
            top = jnp.max(s, axis=1, keepdims=True)
            p = jnp.where(usable, jnp.exp(s - top), 0.0)
            tops.append(top)
            sums.append(jnp.sum(p, axis=1, keepdims=True))
            probs.append(jnp.concatenate([jnp.where(row == b, p, 0.0) for b in range(B)], axis=1))
        probs = jnp.concatenate(probs, axis=0).astype(BF16)
        mixed = jnp.dot(probs, vbuf[l].reshape(B * SEG, HD), preferred_element_type=F32)

        def store_half(phase, start):
            stats = jnp.zeros((B, HD), F32)
            for j in range(4):
                h = start + j
                snd[l, phase, :, j * HD : (j + 1) * HD] = mixed[h * B : (h + 1) * B]
                stats = jnp.where(lane == j, tops[h], stats)
                stats = jnp.where(lane == HALF + j, sums[h], stats)
            snd[l, phase, :, 4 * HD : 5 * HD] = stats

        store_half(4, 0)
        a3 = exchange(l, 4, 5 * HD, along_x)
        store_half(5, 4)
        b3 = exchange(l, 5, 5 * HD, along_y)
        background()
        own = [jnp.zeros((B, HD), F32), jnp.zeros((B, HD), F32)]
        for h in range(8):
            dot = jnp.sum(query[h * B : (h + 1) * B].astype(F32) * new_key, axis=1, keepdims=True)
            own[h // 4] = jnp.where(lane == h % 4, dot * (1.0 / math.sqrt(HD)), own[h // 4])

        def pass_on(phase_in, phase_out):
            joined, top, whole = merge(l, phase_in)
            for j in range(4):
                snd[l, phase_out, :, j * HD : (j + 1) * HD] = joined[j]
            snd[l, phase_out, :, 4 * HD : 5 * HD] = jnp.where(lane < HALF, top, pltpu.roll(whole, HALF, 1))

        arrive(a3)
        pass_on(4, 6)
        a4 = exchange(l, 6, 5 * HD, along_y)
        arrive(b3)
        pass_on(5, 7)
        b4 = exchange(l, 7, 5 * HD, along_x)
        background()
        load[5].wait()
        arrive(a4)
        context = jnp.concatenate(merge(l, 6, (own[0], new_value))[0], axis=1).astype(BF16)
        head_part = jnp.dot(context, wo[l, : 4 * HD, :], preferred_element_type=F32)
        arrive(b4)
        context = jnp.concatenate(merge(l, 7, (own[1], new_value))[0], axis=1).astype(BF16)
        head_part = head_part + jnp.dot(context, wo[l, 4 * HD :, :], preferred_element_type=F32)
        sent += a1 + b1 + a2 + b2 + a3 + b3 + a4 + b4
        return head_part

    def later_layer(l, load, scaled, squares):
        nonlocal sent

        my_cosine, my_sine, within = shared
        raw = jnp.dot(scaled, wqkv[l], preferred_element_type=F32)
        for i in range(10):
            qsnd[l - 1, pl.ds(i, B, stride=16), :] = tile(raw, i)
        qsnd[l - 1, pl.ds(10, B, stride=16), :] = squares
        copies = []
        for d in PLANE_ORDER:
            to = plane[d - 1]
            rows = pl.ds(pl.multiple_of(seat(to[0] // 4, lax.rem(to[0], 4))[1] * 16, 16), 11)
            copy = pltpu.make_async_remote_copy(
                src_ref=qsnd.at[l - 1, rows],
                dst_ref=qrcv.at[l - 1, d - 1, pl.ds(0, 11)],
                send_sem=qssem.at[l - 1, d - 1],
                recv_sem=qrsem.at[l - 1, d - 1],
                device_id=to,
                device_id_type=MESH,
            )
            copy.start()
            copies.append(copy)
        sent += copies
        background()
        narrow(l)
        at = pl.multiple_of(mine * 16, 16)
        heads = [qsnd[l - 1, pl.ds(at, 8), :]]
        others = [qsnd[l - 1, pl.ds(at + 8, 3), :]]
        arrive(copies)
        for d in range(15):
            heads.append(qrcv[l - 1, d, 0:8, :])
            others.append(qrcv[l - 1, d, 8:11, :])
        heads, others = add_up(heads), add_up(others)
        inverse = lax.rsqrt(jnp.sum(others[2:3], axis=1, keepdims=True) / D + EPS)

        def rotate(u, rows):
            u = u * inverse
            return u * my_cosine[:rows] + pltpu.roll(u, HALF, 1) * my_sine[:rows]

        query = rotate(heads, 8).astype(BF16)
        new_key = rotate(jnp.broadcast_to(others[0:1], (B, HD)), 8).astype(BF16).astype(F32)
        new_value = (others[1:2] * inverse).astype(BF16).astype(F32)
        scale = 1.0 / math.sqrt(HD)
        score = jnp.dot(query, keys_t[l], preferred_element_type=F32)
        own = jnp.sum(query.astype(F32) * new_key, axis=1, keepdims=True) * scale
        own = jnp.where(part == 0, own, FILL)
        score = jnp.where(within, score * scale, FILL)
        top = jnp.maximum(jnp.max(score, axis=1, keepdims=True), own)
        p = jnp.where(within, jnp.exp(score - top), 0.0)
        fresh = jnp.where(part == 0, jnp.exp(own - top), 0.0)
        weight = jnp.sum(p, axis=1, keepdims=True) + fresh
        mixed = jnp.dot(p.astype(BF16), values[l - 1], preferred_element_type=F32)
        mixed = mixed + fresh.astype(BF16).astype(F32) * new_value
        stats = jnp.where(lane == row, top, 0.0) + jnp.where(lane == row + HALF, weight, 0.0)
        base = pl.multiple_of(seat_index * 16, 16)
        orcv[l - 1, pl.ds(base, 8), :] = mixed
        orcv[l - 1, pl.ds(base + 8, 1), :] = jnp.sum(stats, axis=0, keepdims=True)
        copies = []
        for d in PLANE_ORDER:
            copy = pltpu.make_async_remote_copy(
                src_ref=orcv.at[l - 1, pl.ds(base, 9)],
                dst_ref=orcv.at[l - 1, pl.ds(base, 9)],
                send_sem=ossem.at[l - 1, d - 1],
                recv_sem=orsem.at[l - 1, d - 1],
                device_id=plane[d - 1],
                device_id_type=MESH,
            )
            copy.start()
            copies.append(copy)
        sent += copies
        background()
        load[5].wait()
        arrive(copies)
        low = orcv[l - 1, pl.ds(8, B, stride=16), :]
        high = orcv[l - 1, pl.ds(128 + 8, B, stride=16), :]
        top = jnp.maximum(low, high)
        scales = [jnp.exp(low - top), jnp.exp(high - top)]
        whole = scales[0] * pltpu.roll(low, HALF, 1) + scales[1] * pltpu.roll(high, HALF, 1)
        scales = [s / whole for s in scales]
        context = []
        for h in range(8):
            context.append(
                jnp.broadcast_to(scales[0][:, h : h + 1], (B, HD)) * orcv[l - 1, pl.ds(h, B, stride=16), :]
                + jnp.broadcast_to(scales[1][:, h : h + 1], (B, HD)) * orcv[l - 1, pl.ds(128 + h, B, stride=16), :]
            )
        context = jnp.concatenate(context, axis=1).astype(BF16)
        return jnp.dot(context, wo[l], preferred_element_type=F32)

    for l in range(LAYERS):
        load = loads[l]
        gain = gbuf[l : l + 1, :].astype(F32)
        scaled = (stream * gain).astype(BF16)
        squares = stream * stream
        squares = (tile(squares, 0) + tile(squares, 1)) + (tile(squares, 2) + tile(squares, 3))
        for i in range(3):
            load[i].wait()
        head_part = (first_layer if l == 0 else later_layer)(l, load, scaled, squares)

        tpb[l, t] = head_part
        copies = []
        for d in (4, 5, 3, 2, 6, 1, 7):
            copy = pltpu.make_async_remote_copy(
                src_ref=tpb.at[l, t],
                dst_ref=tpb.at[l, t],
                send_sem=tssem.at[l, d - 1],
                recv_sem=trsem.at[l, d - 1],
                device_id=along_t[d - 1],
                device_id_type=MESH,
            )
            copy.start()
            copies.append(copy)
        sent += copies
        background()
        arrive(copies)
        stream = stream + add_up([tpb[l, i] for i in range(8)])
    obuf[...] = stream
    result = pltpu.make_async_copy(obuf, out, psem.at[0])
    result.start()
    for l in range(1, LAYERS):
        sent += moves(l)
    for copy in sent:
        copy.wait_send()
    result.wait()


def on_device(hidden, norm_gains, w_query, w_key, w_value, w_out, key_cache, value_cache, lengths):
    exponents = np.arange(HALF, dtype=np.float32) * np.float32(2.0 / HD)
    freq = np.exp(-exponents.astype(np.float64) * math.log(ROPE_BASE)).astype(np.float32)
    freq = jnp.asarray(np.tile(np.concatenate([freq, freq])[None, :], (B, 1)))
    hbm = pl.BlockSpec(memory_space=pl.ANY)
    return pl.pallas_call(
        kernel,
        out_shape=jax.ShapeDtypeStruct((B, 512), F32),
        in_specs=[hbm] * 10,
        out_specs=hbm,
        scratch_shapes=[
            pltpu.VMEM((B, 512), BF16),
            pltpu.VMEM((LAYERS, 512), BF16),
            pltpu.VMEM((LAYERS, 512, 10 * HD), BF16),
            pltpu.VMEM((LAYERS, 8 * HD, 512), BF16),
            pltpu.VMEM((LAYERS, B, SEG, HD), BF16),
            pltpu.VMEM((LAYERS, B, SEG, HD), BF16),
            pltpu.VMEM((B, HD), F32),
            pltpu.VMEM((1, 8, B, PART), F32),
            pltpu.VMEM((1, 8, 3, B, PART), F32),
            pltpu.VMEM((LAYERS, 8, B, 512), F32),
            pltpu.VMEM((LAYERS, HD, B * SEG), BF16),
            pltpu.VMEM((LAYERS - 1, B, 2, SEG, HD), F32),
            pltpu.VMEM((LAYERS - 1, B, 2, SEG, HD), F32),
            pltpu.VMEM((LAYERS - 1, B * SEG, HD), BF16),
            pltpu.VMEM((LAYERS - 1, B * 16, HD), F32),
            pltpu.VMEM((LAYERS - 1, 15, 16, HD), F32),
            pltpu.VMEM((LAYERS - 1, 16 * 16, HD), F32),
            pltpu.VMEM((B, 512), F32),
            pltpu.SMEM((B,), jnp.int32),
            pltpu.SemaphoreType.DMA((LAYERS, 6)),
            pltpu.SemaphoreType.DMA((4,)),
            pltpu.SemaphoreType.DMA((1, 8, 3)),
            pltpu.SemaphoreType.DMA((1, 8, 3)),
            pltpu.SemaphoreType.DMA((LAYERS, 7)),
            pltpu.SemaphoreType.DMA((LAYERS, 7)),
            pltpu.SemaphoreType.DMA((LAYERS - 1, 7)),
            pltpu.SemaphoreType.DMA((LAYERS - 1, 7)),
            pltpu.SemaphoreType.DMA((LAYERS - 1, 15)),
            pltpu.SemaphoreType.DMA((LAYERS - 1, 15)),
            pltpu.SemaphoreType.DMA((LAYERS - 1, 15)),
            pltpu.SemaphoreType.DMA((LAYERS - 1, 15)),
        ],
        compiler_params=pltpu.CompilerParams(
            collective_id=0, has_side_effects=True, vmem_limit_bytes=60 * 1024 * 1024
        ),
    )(hidden, norm_gains, w_query, w_key, w_value, w_out, key_cache, value_cache, lengths, freq)


def solution(mesh):
    return jax.shard_map(
        on_device,
        mesh=mesh,
        in_specs=(
            P(None, "ctx"),
            P(None, "ctx"),
            P(None, "ctx", "tp"),
            P(None, "ctx", "tp"),
            P(None, "ctx", "tp"),
            P(None, "tp", "ctx"),
            P(None, None, "tp", "ctx", None),
            P(None, None, "tp", "ctx", None),
            P(),
        ),
        out_specs=P(None, "ctx"),
        check_vma=False,
    )
```

```python
import functools
import math

import jax
import jax.numpy as jnp
import numpy as np
from jax import lax
from jax.experimental import pallas as pl
from jax.experimental.pallas import tpu as pltpu
from jax.sharding import PartitionSpec as P

MESH = pl.DeviceIdType.MESH
LAYERS = 4
B = 8
HD = 128
HALF = 64
D = 8192
SEG = 128
FILL = -1e30
EPS = 1e-5
ROPE_BASE = 500000.0
F32 = jnp.float32
BF16 = jnp.bfloat16
QA = 5 * HD
QB = 5 * HD
PART = 6 * HD
PLANE_ORDER = (10, 6, 9, 11, 14, 2, 8, 5, 7, 13, 15, 1, 3, 4, 12)
UNIT = 32
SHIFTS = ((1, 0), (2, 0), (3, 0), (0, 1), (1, 1), (2, 1), (3, 1))
NEAR, FAR = (0, 2, 3, 1), (4, 6, 5)
PLAN = (
    (1, 1, 1, 1, 4, 2, 2, 4, 2, 2, 4, 0, 0, 0),
    (0, 0, 2, 2, 4, 2, 2, 4, 2, 2, 4, 0, 0, 0),
)


def tile(value, i):
    return value[:, i * HD : (i + 1) * HD]


def add_up(terms):
    while len(terms) > 1:
        pairs = [terms[i] + terms[i + 1] for i in range(0, len(terms) - 1, 2)]
        terms = pairs + terms[len(terms) - len(terms) % 2 :]
    return terms[0]


def kernel(
    hidden, gains, w_query, w_key, w_value, w_out, key_cache, value_cache, lengths_in, freq,
    out,
    hbuf, gbuf, wqkv, wo, kbuf, vbuf, fbuf, snd, rcv, tpb, keys_t, stage, moved, values, qsnd, qrcv, orcv, obuf, lengths,
    lsem, psem, ssem, rsem, tssem, trsem, bssem, brsem, qssem, qrsem, ossem, orsem,
):
    c = lax.axis_index("ctx")
    t = lax.axis_index("tp")
    y, x = c // 4, lax.rem(c, 4)
    core = lax.rem(t, 2)

    def seat(y, x):
        u, v = x + core * (y - x), y + core * (x - y)
        return v // 2, lax.rem(v, 2) * 4 + u

    def place(part, sequence):
        u, v = lax.rem(sequence, 4), part * 2 + sequence // 4
        return (v + core * (u - v)) * 4 + u + core * (v - u)

    part, mine = seat(y, x)
    seat_index = part * 8 + mine

    def weight_loads(l):
        return (
            pltpu.make_async_copy(w_query.at[l], wqkv.at[l, :, pl.ds(0, 8 * HD)], lsem.at[l, 0]),
            pltpu.make_async_copy(w_key.at[l], wqkv.at[l, :, pl.ds(8 * HD, HD)], lsem.at[l, 1]),
            pltpu.make_async_copy(w_value.at[l], wqkv.at[l, :, pl.ds(9 * HD, HD)], lsem.at[l, 2]),
            pltpu.make_async_copy(key_cache.at[l, :, 0], kbuf.at[l], lsem.at[l, 3]),
            pltpu.make_async_copy(value_cache.at[l, :, 0], vbuf.at[l], lsem.at[l, 4]),
            pltpu.make_async_copy(w_out.at[l], wo.at[l], lsem.at[l, 5]),
        )

    small = (
        pltpu.make_async_copy(hidden, hbuf, psem.at[0]),
        pltpu.make_async_copy(gains, gbuf, psem.at[1]),
        pltpu.make_async_copy(freq, fbuf, psem.at[2]),
        pltpu.make_async_copy(lengths_in, lengths, psem.at[3]),
    )
    along_x = [(y * 4 + lax.rem(x + d, 4), t) for d in (1, 2, 3)]
    along_y = [(lax.rem(y + d, 4) * 4 + x, t) for d in (1, 2, 3)]
    along_t = [(c, lax.rem(t + d, 8)) for d in range(1, 8)]
    plane = [(lax.rem(y + d // 4, 4) * 4 + lax.rem(x + d % 4, 4), t) for d in range(1, 16)]
    barrier = pltpu.get_barrier_semaphore()
    for peer in along_x + along_y + along_t:
        pl.semaphore_signal(barrier, inc=1, device_id=peer, device_id_type=MESH)
    for copy in small:
        copy.start()
    loads = [weight_loads(l) for l in range(LAYERS)]
    for copy in loads[0][:3]:
        copy.start()

    lane = lax.broadcasted_iota(jnp.int32, (B, HD), 1)
    row = lax.broadcasted_iota(jnp.int32, (B, HD), 0)
    def positions():
        small[3].wait()
        length = jnp.zeros((B, HD), jnp.int32)
        for b in range(B):
            length = jnp.where(row == b, lengths[b], length)
        usable = c * SEG + lane < length
        my_length = lengths[mine]
        small[2].wait()

        def angles(positions):
            angle = positions.astype(F32) * fbuf[...]
            sine = jnp.sin(angle)
            return jnp.cos(angle), jnp.where(lane < HALF, -sine, sine)

        cosine, sine = angles(length)
        my_cosine, my_sine = angles(jnp.full((B, HD), my_length, jnp.int32))
        held = jnp.concatenate([place(part, s) * SEG + lane for s in range(B)], axis=1)
        within = held < my_length
        return usable, cosine, sine, my_cosine, my_sine, within

    small[0].wait()
    small[1].wait()
    stream = hbuf[...].astype(F32)

    def exchange(l, phase, width, peers):
        copies = []
        for i in (1, 0, 2):
            copy = pltpu.make_async_remote_copy(
                src_ref=snd.at[l, phase, :, pl.ds(0, width)],
                dst_ref=rcv.at[l, phase, i, :, pl.ds(0, width)],
                send_sem=ssem.at[l, phase, i],
                recv_sem=rsem.at[l, phase, i],
                device_id=peers[i],
                device_id_type=MESH,
            )
            copy.start()
            copies.append(copy)
        return copies

    def arrive(copies):
        for copy in copies:
            copy.wait_recv()

    def total(l, phase, width):
        own = snd[l, phase, :, :width]
        got = [rcv[l, phase, i, :, :width] for i in range(3)]
        return (own + got[0]) + (got[1] + got[2])

    def merge(l, phase, fresh=None):
        outs = [snd[l, phase, :, : 4 * HD]] + [rcv[l, phase, i, :, : 4 * HD] for i in range(3)]
        stats = [snd[l, phase, :, 4 * HD : 5 * HD]] + [
            rcv[l, phase, i, :, 4 * HD : 5 * HD] for i in range(3)
        ]
        sums = [pltpu.roll(s, HALF, 1) for s in stats]
        top = jnp.maximum(jnp.maximum(stats[0], stats[1]), jnp.maximum(stats[2], stats[3]))
        if fresh is not None:
            top = jnp.maximum(top, fresh[0])
        scale = [jnp.exp(s - top) for s in stats]
        whole = (scale[0] * sums[0] + scale[1] * sums[1]) + (scale[2] * sums[2] + scale[3] * sums[3])
        if fresh is not None:
            new = jnp.exp(fresh[0] - top)
            whole = whole + new
            scale = [s / whole for s in scale]
            new = new.astype(BF16).astype(F32) / whole
        result = []
        for j in range(4):
            parts = [jnp.broadcast_to(s[:, j : j + 1], (B, HD)) * tile(o, j) for s, o in zip(scale, outs)]
            joined = (parts[0] + parts[1]) + (parts[2] + parts[3])
            if fresh is not None:
                joined = joined + jnp.broadcast_to(new[:, j : j + 1], (B, HD)) * fresh[1]
            result.append(joined)
        return result, top, whole


    def widen(l):
        loads[l][3].wait()
        loads[l][4].wait()
        for b in range(B):
            stage[l - 1, b, 0] = kbuf[l, b].astype(F32)
            stage[l - 1, b, 1] = vbuf[l, b].astype(F32)
        moved[l - 1, mine, 0] = stage[l - 1, mine, 0]
        moved[l - 1, mine, 1] = stage[l - 1, mine, 1]

    def shifted(dx, other, sign=1):
        return lax.rem(mine // 4 + other, 2) * 4 + lax.rem(lax.rem(mine, 4) + 4 + sign * dx, 4)

    def moved_copy(l, j, to, src, dst):
        return pltpu.make_async_remote_copy(
            src_ref=src,
            dst_ref=dst,
            send_sem=bssem.at[l - 1, j],
            recv_sem=brsem.at[l - 1, j],
            device_id=(place(part, to), t),
            device_id_type=MESH,
        )

    def move(l, unit, group):
        which, rows = unit // (SEG // UNIT), pl.ds(unit % (SEG // UNIT) * UNIT, UNIT)
        for j in group:
            to = shifted(*SHIFTS[j])
            moved_copy(
                l, j, to, stage.at[l - 1, to, which, rows], moved.at[l - 1, mine, which, rows]
            ).start()

    def moves(l):
        result = []
        for j in range(7):
            to, origin = shifted(*SHIFTS[j]), shifted(*SHIFTS[j], sign=-1)
            result.append(moved_copy(l, j, to, stage.at[l - 1, to], moved.at[l - 1, origin]))
        return result

    def narrow(l):
        for queue, group in ((near, NEAR), (far, FAR)):
            units(queue, sum(item[0] <= l for item in queue), group)
        arrive(moves(l))
        for s in range(8):
            keys_t[l, :, s * SEG : (s + 1) * SEG] = moved[l - 1, s, 0].T.astype(BF16)
            values[l - 1, s * SEG : (s + 1) * SEG] = moved[l - 1, s, 1].astype(BF16)

    widened = []

    def units(queue, count, group):
        for _ in range(min(count, len(queue))):
            l, u = queue.pop(0)
            if l not in widened:
                widened.append(l)
                widen(l)
            move(l, u, group)

    every = [(l, u) for l in range(1, LAYERS) for u in range(2 * SEG // UNIT)]
    near, far = list(every), list(every)

    def background():
        units(near, PLAN[0][len(steps)], NEAR)
        units(far, PLAN[1][len(steps)], FAR)
        steps.append(1)

    steps = []
    shared = []
    sent = []

    def first_layer(l, load, scaled, squares):
        nonlocal sent
        snd[l, 0, :, :QA] = jnp.dot(scaled, wqkv[l, :, :QA], preferred_element_type=F32)
        snd[l, 0, :, QA : QA + HD] = squares
        snd[l, 1, :, :QB] = jnp.dot(scaled, wqkv[l, :, QA:], preferred_element_type=F32)
        pl.semaphore_wait(barrier, 13)
        a1 = exchange(l, 0, QA + HD, along_x)
        b1 = exchange(l, 1, QB, along_y)
        for copy in loads[0][3:]:
            copy.start()
        for group in loads[1:]:
            for copy in group:
                copy.start()
        usable, cosine, sine, my_cosine, my_sine, within = known = positions()
        shared.extend(known[3:])
        load[3].wait()
        load[4].wait()
        for b in range(B):
            keys_t[0, :, b * SEG : (b + 1) * SEG] = kbuf[0, b].astype(F32).T.astype(BF16)
        background()
        arrive(a1)
        snd[l, 2, :, : QA + HD] = total(l, 0, QA + HD)
        a2 = exchange(l, 2, QA + HD, along_y)
        arrive(b1)
        snd[l, 3, :, :QB] = total(l, 1, QB)
        b2 = exchange(l, 3, QB, along_x)
        background()
        arrive(a2)
        first = total(l, 2, QA + HD)
        inverse = lax.rsqrt(jnp.sum(tile(first, 5), axis=1, keepdims=True) / D + EPS)
        cos_l, sin_l = cosine * inverse, sine * inverse

        def rotate(u):
            return u * cos_l + pltpu.roll(u, HALF, 1) * sin_l

        arrive(b2)
        second = total(l, 3, QB)
        raw = [tile(first, i) for i in range(5)] + [tile(second, i) for i in range(3)]
        query = jnp.concatenate([rotate(u) for u in raw], axis=0).astype(BF16)
        new_key = rotate(tile(second, 3)).astype(BF16).astype(F32)
        new_value = (tile(second, 4) * inverse).astype(BF16).astype(F32)

        score = jnp.dot(query, keys_t[l], preferred_element_type=F32)
        probs, tops, sums = [], [], []
        for h in range(8):
            block = score[h * B : (h + 1) * B]
            s = tile(block, 0)
            for b in range(1, B):
                s = jnp.where(row == b, tile(block, b), s)
            s = jnp.where(usable, s * (1.0 / math.sqrt(HD)), FILL)
            top = jnp.max(s, axis=1, keepdims=True)
            p = jnp.where(usable, jnp.exp(s - top), 0.0)
            tops.append(top)
            sums.append(jnp.sum(p, axis=1, keepdims=True))
            probs.append(jnp.concatenate([jnp.where(row == b, p, 0.0) for b in range(B)], axis=1))
        probs = jnp.concatenate(probs, axis=0).astype(BF16)
        mixed = jnp.dot(probs, vbuf[l].reshape(B * SEG, HD), preferred_element_type=F32)

        def store_half(phase, start):
            stats = jnp.zeros((B, HD), F32)
            for j in range(4):
                h = start + j
                snd[l, phase, :, j * HD : (j + 1) * HD] = mixed[h * B : (h + 1) * B]
                stats = jnp.where(lane == j, tops[h], stats)
                stats = jnp.where(lane == HALF + j, sums[h], stats)
            snd[l, phase, :, 4 * HD : 5 * HD] = stats

        store_half(4, 0)
        a3 = exchange(l, 4, 5 * HD, along_x)
        store_half(5, 4)
        b3 = exchange(l, 5, 5 * HD, along_y)
        background()
        own = [jnp.zeros((B, HD), F32), jnp.zeros((B, HD), F32)]
        for h in range(8):
            dot = jnp.sum(query[h * B : (h + 1) * B].astype(F32) * new_key, axis=1, keepdims=True)
            own[h // 4] = jnp.where(lane == h % 4, dot * (1.0 / math.sqrt(HD)), own[h // 4])

        def pass_on(phase_in, phase_out):
            joined, top, whole = merge(l, phase_in)
            for j in range(4):
                snd[l, phase_out, :, j * HD : (j + 1) * HD] = joined[j]
            snd[l, phase_out, :, 4 * HD : 5 * HD] = jnp.where(lane < HALF, top, pltpu.roll(whole, HALF, 1))

        arrive(a3)
        pass_on(4, 6)
        a4 = exchange(l, 6, 5 * HD, along_y)
        arrive(b3)
        pass_on(5, 7)
        b4 = exchange(l, 7, 5 * HD, along_x)
        background()
        load[5].wait()
        arrive(a4)
        context = jnp.concatenate(merge(l, 6, (own[0], new_value))[0], axis=1).astype(BF16)
        head_part = jnp.dot(context, wo[l, : 4 * HD, :], preferred_element_type=F32)
        arrive(b4)
        context = jnp.concatenate(merge(l, 7, (own[1], new_value))[0], axis=1).astype(BF16)
        head_part = head_part + jnp.dot(context, wo[l, 4 * HD :, :], preferred_element_type=F32)
        sent += a1 + b1 + a2 + b2 + a3 + b3 + a4 + b4
        return head_part

    def later_layer(l, load, scaled, squares):
        nonlocal sent

        my_cosine, my_sine, within = shared
        raw = jnp.dot(scaled, wqkv[l], preferred_element_type=F32)
        for i in range(10):
            qsnd[l - 1, pl.ds(i, B, stride=16), :] = tile(raw, i)
        qsnd[l - 1, pl.ds(10, B, stride=16), :] = squares
        copies = []
        for d in PLANE_ORDER:
            to = plane[d - 1]
            rows = pl.ds(pl.multiple_of(seat(to[0] // 4, lax.rem(to[0], 4))[1] * 16, 16), 11)
            copy = pltpu.make_async_remote_copy(
                src_ref=qsnd.at[l - 1, rows],
                dst_ref=qrcv.at[l - 1, d - 1, pl.ds(0, 11)],
                send_sem=qssem.at[l - 1, d - 1],
                recv_sem=qrsem.at[l - 1, d - 1],
                device_id=to,
                device_id_type=MESH,
            )
            copy.start()
            copies.append(copy)
        sent += copies
        background()
        narrow(l)
        at = pl.multiple_of(mine * 16, 16)
        heads = [qsnd[l - 1, pl.ds(at, 8), :]]
        others = [qsnd[l - 1, pl.ds(at + 8, 3), :]]
        arrive(copies)
        for d in range(15):
            heads.append(qrcv[l - 1, d, 0:8, :])
            others.append(qrcv[l - 1, d, 8:11, :])
        heads, others = add_up(heads), add_up(others)
        inverse = lax.rsqrt(jnp.sum(others[2:3], axis=1, keepdims=True) / D + EPS)

        def rotate(u, rows):
            u = u * inverse
            return u * my_cosine[:rows] + pltpu.roll(u, HALF, 1) * my_sine[:rows]

        query = rotate(heads, 8).astype(BF16)
        new_key = rotate(jnp.broadcast_to(others[0:1], (B, HD)), 8).astype(BF16).astype(F32)
        new_value = (others[1:2] * inverse).astype(BF16).astype(F32)
        scale = 1.0 / math.sqrt(HD)
        score = jnp.dot(query, keys_t[l], preferred_element_type=F32)
        own = jnp.sum(query.astype(F32) * new_key, axis=1, keepdims=True) * scale
        own = jnp.where(part == 0, own, FILL)
        score = jnp.where(within, score * scale, FILL)
        top = jnp.maximum(jnp.max(score, axis=1, keepdims=True), own)
        p = jnp.where(within, jnp.exp(score - top), 0.0)
        fresh = jnp.where(part == 0, jnp.exp(own - top), 0.0)
        weight = jnp.sum(p, axis=1, keepdims=True) + fresh
        mixed = jnp.dot(p.astype(BF16), values[l - 1], preferred_element_type=F32)
        mixed = mixed + fresh.astype(BF16).astype(F32) * new_value
        stats = jnp.where(lane == row, top, 0.0) + jnp.where(lane == row + HALF, weight, 0.0)
        base = pl.multiple_of(seat_index * 16, 16)
        orcv[l - 1, pl.ds(base, 8), :] = mixed
        orcv[l - 1, pl.ds(base + 8, 1), :] = jnp.sum(stats, axis=0, keepdims=True)
        copies = []
        for d in PLANE_ORDER:
            copy = pltpu.make_async_remote_copy(
                src_ref=orcv.at[l - 1, pl.ds(base, 9)],
                dst_ref=orcv.at[l - 1, pl.ds(base, 9)],
                send_sem=ossem.at[l - 1, d - 1],
                recv_sem=orsem.at[l - 1, d - 1],
                device_id=plane[d - 1],
                device_id_type=MESH,
            )
            copy.start()
            copies.append(copy)
        sent += copies
        background()
        load[5].wait()
        arrive(copies)
        low = orcv[l - 1, pl.ds(8, B, stride=16), :]
        high = orcv[l - 1, pl.ds(128 + 8, B, stride=16), :]
        top = jnp.maximum(low, high)
        scales = [jnp.exp(low - top), jnp.exp(high - top)]
        whole = scales[0] * pltpu.roll(low, HALF, 1) + scales[1] * pltpu.roll(high, HALF, 1)
        scales = [s / whole for s in scales]
        context = []
        for h in range(8):
            context.append(
                jnp.broadcast_to(scales[0][:, h : h + 1], (B, HD)) * orcv[l - 1, pl.ds(h, B, stride=16), :]
                + jnp.broadcast_to(scales[1][:, h : h + 1], (B, HD)) * orcv[l - 1, pl.ds(128 + h, B, stride=16), :]
            )
        context = jnp.concatenate(context, axis=1).astype(BF16)
        return jnp.dot(context, wo[l], preferred_element_type=F32)

    for l in range(LAYERS):
        load = loads[l]
        gain = gbuf[l : l + 1, :].astype(F32)
        scaled = (stream * gain).astype(BF16)
        squares = stream * stream
        squares = (tile(squares, 0) + tile(squares, 1)) + (tile(squares, 2) + tile(squares, 3))
        for i in range(3):
            load[i].wait()
        head_part = (first_layer if l == 0 else later_layer)(l, load, scaled, squares)

        tpb[l, t] = head_part
        copies = []
        for d in (4, 5, 3, 2, 6, 1, 7):
            copy = pltpu.make_async_remote_copy(
                src_ref=tpb.at[l, t],
                dst_ref=tpb.at[l, t],
                send_sem=tssem.at[l, d - 1],
                recv_sem=trsem.at[l, d - 1],
                device_id=along_t[d - 1],
                device_id_type=MESH,
            )
            copy.start()
            copies.append(copy)
        sent += copies
        background()
        arrive(copies)
        stream = stream + add_up([tpb[l, i] for i in range(8)])
    obuf[...] = stream
    result = pltpu.make_async_copy(obuf, out, psem.at[0])
    result.start()
    for l in range(1, LAYERS):
        sent += moves(l)
    for copy in sent:
        copy.wait_send()
    result.wait()


def on_device(hidden, norm_gains, w_query, w_key, w_value, w_out, key_cache, value_cache, lengths):
    exponents = np.arange(HALF, dtype=np.float32) * np.float32(2.0 / HD)
    freq = np.exp(-exponents.astype(np.float64) * math.log(ROPE_BASE)).astype(np.float32)
    freq = jnp.asarray(np.tile(np.concatenate([freq, freq])[None, :], (B, 1)))
    hbm = pl.BlockSpec(memory_space=pl.ANY)
    return pl.pallas_call(
        kernel,
        out_shape=jax.ShapeDtypeStruct((B, 512), F32),
        in_specs=[hbm] * 10,
        out_specs=hbm,
        scratch_shapes=[
            pltpu.VMEM((B, 512), BF16),
            pltpu.VMEM((LAYERS, 512), BF16),
            pltpu.VMEM((LAYERS, 512, 10 * HD), BF16),
            pltpu.VMEM((LAYERS, 8 * HD, 512), BF16),
            pltpu.VMEM((LAYERS, B, SEG, HD), BF16),
            pltpu.VMEM((LAYERS, B, SEG, HD), BF16),
            pltpu.VMEM((B, HD), F32),
            pltpu.VMEM((1, 8, B, PART), F32),
            pltpu.VMEM((1, 8, 3, B, PART), F32),
            pltpu.VMEM((LAYERS, 8, B, 512), F32),
            pltpu.VMEM((LAYERS, HD, B * SEG), BF16),
            pltpu.VMEM((LAYERS - 1, B, 2, SEG, HD), F32),
            pltpu.VMEM((LAYERS - 1, B, 2, SEG, HD), F32),
            pltpu.VMEM((LAYERS - 1, B * SEG, HD), BF16),
            pltpu.VMEM((LAYERS - 1, B * 16, HD), F32),
            pltpu.VMEM((LAYERS - 1, 15, 16, HD), F32),
            pltpu.VMEM((LAYERS - 1, 16 * 16, HD), F32),
            pltpu.VMEM((B, 512), F32),
            pltpu.SMEM((B,), jnp.int32),
            pltpu.SemaphoreType.DMA((LAYERS, 6)),
            pltpu.SemaphoreType.DMA((4,)),
            pltpu.SemaphoreType.DMA((1, 8, 3)),
            pltpu.SemaphoreType.DMA((1, 8, 3)),
            pltpu.SemaphoreType.DMA((LAYERS, 7)),
            pltpu.SemaphoreType.DMA((LAYERS, 7)),
            pltpu.SemaphoreType.DMA((LAYERS - 1, 7)),
            pltpu.SemaphoreType.DMA((LAYERS - 1, 7)),
            pltpu.SemaphoreType.DMA((LAYERS - 1, 15)),
            pltpu.SemaphoreType.DMA((LAYERS - 1, 15)),
            pltpu.SemaphoreType.DMA((LAYERS - 1, 15)),
            pltpu.SemaphoreType.DMA((LAYERS - 1, 15)),
        ],
        compiler_params=pltpu.CompilerParams(
            collective_id=0, has_side_effects=True, vmem_limit_bytes=60 * 1024 * 1024
        ),
    )(hidden, norm_gains, w_query, w_key, w_value, w_out, key_cache, value_cache, lengths, freq)


def solution(mesh):
    return jax.shard_map(
        on_device,
        mesh=mesh,
        in_specs=(
            P(None, "ctx"),
            P(None, "ctx"),
            P(None, "ctx", "tp"),
            P(None, "ctx", "tp"),
            P(None, "ctx", "tp"),
            P(None, "tp", "ctx"),
            P(None, None, "tp", "ctx", None),
            P(None, None, "tp", "ctx", None),
            P(),
        ),
        out_specs=P(None, "ctx"),
        check_vma=False,
    )
```
